32 devices in a mesh: parts: 2 (over y), row: 16 (over z, x, core).
Axes of the slice: x: 2, y: 2, z: 4, core: 2. Of those that a mesh axis runs over, the one named last changes fastest.
Arguments:
- tokens: bfloat16 [64, 256, 768], P(('parts', 'row')), parts along dimension 0, may hold values from -6 to 6
- w_query: bfloat16 [768, 768], replicated, may hold values from -0.21875 to 0.21875
- w_key: bfloat16 [768, 768], replicated, may hold values from -0.21875 to 0.21875
- w_value: bfloat16 [768, 768], replicated, may hold values from -0.21875 to 0.21875
- w_out: bfloat16 [768, 768], replicated, may hold values from -0.21875 to 0.21875
- omega: bfloat16 [12, 64, 256], replicated, may hold values from -5 to 5
- conv_kernel: float32 [3, 3, 768], replicated, may hold values from -0.6 to 0.6
- norm_gain: float32 [768], replicated, may hold values from 0.1 to 1.9
Outputs:
- layer_out: bfloat16 [64, 256, 768], P(('parts', 'row')), parts along dimension 0
The draws below stay inside these ranges and needn't reach their ends.
There are 2 independent parts, one for each index of `parts`. The reference program is written for one: setup_inputs(seed, part) draws one part's arguments, and reference() takes and returns one part's arrays. A program takes and returns all parts, laid end to end along the dimension named above; an argument that names none is the same for every part. Nothing has to cross between parts.
All inputs are finite; a program needn't handle non-finite values.
Results may differ from the reference program's by a relative error of at most 0.0081.
Values may be sent and summed in bfloat16 or wider, within the bound.
No kernel may reach another device: no remote copies, remote signals or barrier semaphores. Data moves between devices by JAX's collectives and lax.ppermute only.
A program may use at most 64 MiB of HBM per device.

```python
import jax
import jax.numpy as jnp
from jax import lax

D = 768
HEADS = 12
DH = 64
FEAT = 256
COLS = 256
ROWS_DEV = 2
GRID_ROWS = 32


def block_scale(stream_key, shape, split, low, high):
    def one(dim, shards_of):
        heights = jax.random.uniform(jax.random.fold_in(jax.random.fold_in(stream_key, 6), dim), (shards_of,), jnp.float32, low / len(split), high / len(split))
        return jnp.repeat(jnp.exp(heights), shape[dim] // shards_of).reshape((-1,) + (1,) * (len(shape) - dim - 1))

    factor_of = one(*split[0])
    for cut in split[1:]:
        factor_of = factor_of * one(*cut)
    return factor_of


def centred(stream_key, dims, scale, bound, shards=(), held_as=jnp.bfloat16):
    gain = block_scale(stream_key, dims, shards, -0.22, 0.18) if shards else 1.0
    values = jax.random.normal(stream_key, dims, jnp.float32) * scale * gain
    return jnp.minimum(jnp.maximum(values, -bound), bound).astype(held_as)


def setup_inputs(seed: int = 0, part: int = 0) -> dict:
    streams_of = jax.random.split(jax.random.key(seed), 9)
    own_keys = jax.random.split(jax.random.fold_in(streams_of[8], part), 9)
    tokens = centred(own_keys[0], (GRID_ROWS, COLS, D), 1.0, 6.0, ((0, 16),))
    w_query = centred(streams_of[1], (D, D), D ** -0.5, 0.21875)
    w_key = centred(streams_of[2], (D, D), D ** -0.5, 0.21875)
    w_value = centred(streams_of[3], (D, D), D ** -0.5, 0.21875)
    w_out = centred(streams_of[4], (D, D), D ** -0.5, 0.21875)
    omega = centred(streams_of[5], (HEADS, DH, FEAT), 1.0, 5.0)
    conv_kernel = jnp.clip(jax.random.uniform(streams_of[6], (3, 3, D), jnp.float32, -0.6, 0.6), -0.6, 0.6)
    norm_gain = jnp.clip(1.0 + 0.18 * jax.random.normal(streams_of[7], (D,), jnp.float32), 0.1, 1.9)
    return {"tokens": tokens, "w_query": w_query, "w_key": w_key, "w_value": w_value, "w_out": w_out, "omega": omega, "conv_kernel": conv_kernel, "norm_gain": norm_gain}


def project(rows, weight):
    return jnp.dot(rows, weight, preferred_element_type=jnp.float32).astype(jnp.bfloat16)

def feature_map(heads_in, omega):
    dim_head = heads_in.shape[-1]
    values = heads_in.astype(jnp.float32)
    lifted = jnp.einsum('thd,hdf->thf', values, omega.astype(jnp.float32))
    square = lax.optimization_barrier(jnp.sum(values * values, axis=-1, keepdims=True))
    feats = jnp.exp(lifted * dim_head ** (-0.25) - square * 0.5 * dim_head ** (-0.5)) * omega.shape[-1] ** (-0.5)
    return feats.astype(jnp.bfloat16)

def reference(tokens, w_query, w_key, w_value, w_out, omega, conv_kernel, norm_gain):
    grid_rows, cols, width = tokens.shape
    heads, dim_head, nfeat = omega.shape
    blocks = grid_rows // ROWS_DEV
    flat = tokens.reshape(grid_rows * cols, width)
    value = project(flat, w_value)
    value_blocks = value.reshape(blocks, ROWS_DEV * cols, heads, dim_head)
    token_blocks = tokens.reshape(blocks, ROWS_DEV * cols, width)

    def add_state(carry, pair):
        rows, vals = pair
        feat_key = feature_map(project(rows, w_key).reshape(-1, heads, dim_head), omega).astype(jnp.float32)
        state = carry[0] + jnp.einsum('thf,thd->fhd', feat_key, vals.astype(jnp.float32))
        total = carry[1] + lax.optimization_barrier(jnp.sum(feat_key, axis=0)).astype(jnp.float32)
        return ((state, total), None)
    init = (jnp.zeros((nfeat, heads, dim_head), jnp.float32), jnp.zeros((heads, nfeat), jnp.float32))
    (kv_sum, key_sum), unused = lax.scan(add_state, init, (token_blocks, value_blocks))
    kv_state = kv_sum.astype(jnp.bfloat16).astype(jnp.float32)
    padded = jnp.pad(value.reshape(grid_rows, cols, width).astype(jnp.float32), ((1, 1), (1, 1), (0, 0)))
    position = jnp.zeros((grid_rows, cols, width), jnp.float32)
    for shift_a in range(3):
        for shift_b in range(3):
            position = position + padded[shift_a:shift_a + grid_rows, shift_b:shift_b + cols, :] * conv_kernel[shift_a, shift_b]
    position_blocks = position.reshape(blocks, ROWS_DEV * cols, width)

    def block_out(pair):
        rows, local_pos = pair
        feat_query = feature_map(project(rows, w_query).reshape(-1, heads, dim_head), omega).astype(jnp.float32)
        numer = jnp.einsum('thf,fhd->thd', feat_query, kv_state, precision=lax.Precision.HIGHEST)
        denom = jnp.einsum('thf,hf->th', feat_query, key_sum, precision=lax.Precision.HIGHEST)
        attn = numer / denom[:, :, None]
        scale = lax.rsqrt(lax.optimization_barrier(jnp.mean(attn * attn, axis=(1, 2), keepdims=True)) + 1e-06)
        normed = (attn * scale).reshape(-1, width) * norm_gain
        mixed = (normed + local_pos).astype(jnp.bfloat16)
        out = rows.astype(jnp.float32) + jnp.dot(mixed, w_out, preferred_element_type=jnp.float32)
        return out.astype(jnp.bfloat16)
    outs = lax.map(block_out, (token_blocks, position_blocks))
    return outs.reshape(grid_rows, cols, width)
```

```python
import functools

import jax
import jax.numpy as jnp
from jax import lax
from jax.experimental import pallas as pl
from jax.experimental.pallas import tpu as pltpu
from jax.sharding import PartitionSpec as P

BF = jnp.bfloat16
F32 = jnp.float32
LOG2E = 1.4426950408889634
VMEM_LIMIT = 28 * 1024 * 1024


def vmem_specs(count):
    return [pl.BlockSpec(memory_space=pltpu.VMEM)] * count


def tiles_of(total, wanted):
    return wanted if total % wanted == 0 else total


def feature_tile(proj, omega_pair, ones_pair, dim_head, nfeat):
    rows = proj.shape[0]
    wide = 2 * dim_head
    lifted = jnp.dot(proj, omega_pair, preferred_element_type=F32)
    values = proj.astype(F32)
    square = values * values * (0.5 * dim_head ** (-0.5) * LOG2E)
    high = square.astype(BF)
    low = (square - high.astype(F32)).astype(BF)
    summed = jnp.dot(jnp.concatenate([high, low], axis=1), ones_pair, preferred_element_type=F32)
    halves = []
    shift = 0.5 * jnp.log2(jnp.float32(nfeat))
    for head in range(2):
        drop = summed[:, head * wide : (head + 1) * wide] + shift
        for part in range(nfeat // wide):
            start = head * nfeat + part * wide
            grown = lifted[:, start : start + wide] * (dim_head ** (-0.25) * LOG2E)
            halves.append(jnp.exp2(grown - drop).astype(BF))
    return jnp.concatenate(halves, axis=1)


def fill_pairs(omega_ref, pair_ref, ones_ref):
    heads, dim_head, nfeat = omega_ref.shape
    pair_ref[...] = jnp.zeros_like(pair_ref)
    for head in range(heads):
        side = head % 2
        pair_ref[head // 2, side * dim_head : (side + 1) * dim_head, side * nfeat : (side + 1) * nfeat] = omega_ref[head]
    shape = ones_ref.shape
    row = lax.broadcasted_iota(jnp.int32, shape, 0) // dim_head % 2
    col = lax.broadcasted_iota(jnp.int32, shape, 1) // (2 * dim_head)
    ones_ref[...] = jnp.where(row == col, 1.0, 0.0).astype(BF)


def state_kernel(flip_ref, x_ref, wk_ref, wv_ref, omega_ref, state_ref, value_ref, pair_ref, ones_ref, vt_ref, feat_ref):
    heads, dim_head, nfeat = omega_ref.shape
    tokens, width = x_ref.shape
    half = heads // 2
    fill_pairs(omega_ref, pair_ref, ones_ref)
    x = x_ref[...]
    value = jnp.dot(x, wv_ref[...], preferred_element_type=F32).astype(BF)
    value_ref[...] = value
    turned = value.T
    mark = lax.broadcasted_iota(jnp.int32, (16, tokens), 0)
    for head in range(heads):
        vt_ref[head, :dim_head, :] = turned[head * dim_head : (head + 1) * dim_head]
        vt_ref[head, dim_head:, :] = jnp.where(mark == head % half, 1.0, 0.0).astype(BF)
    rows = tiles_of(tokens, 128)
    chunk = 4 * dim_head
    sums = None
    for first in range(0, heads, 4):
        count = min(4, heads - first)
        key = jnp.dot(x, wk_ref[:, first * dim_head : (first + count) * dim_head], preferred_element_type=F32).astype(BF)
        for pair in range(count // 2):
            which = first // 2 + pair
            for start in range(0, tokens, rows):
                proj = key[start : start + rows, pair * 2 * dim_head : (pair + 1) * 2 * dim_head]
                feat_ref[start : start + rows, :] = feature_tile(proj, pair_ref[which], ones_ref[...], dim_head, nfeat)
            for side in range(2):
                head = 2 * which + side
                local = jnp.dot(vt_ref[head], feat_ref[:, side * nfeat : (side + 1) * nfeat], preferred_element_type=F32)
                slot = lax.rem(flip_ref[0] + head // half, 2)
                place = head % half
                state_ref[slot, place * dim_head : (place + 1) * dim_head, :] = local[:dim_head].astype(BF)
                sums = local[dim_head:] if place == 0 else sums + local[dim_head:]
                if place == half - 1:
                    state_ref[slot, half * dim_head :, :] = sums.astype(BF)


def query_kernel(x_ref, wq_ref, omega_ref, feat_ref, pair_ref, ones_ref):
    heads, dim_head, nfeat = omega_ref.shape
    tokens = x_ref.shape[0]
    fill_pairs(omega_ref, pair_ref, ones_ref)
    rows = tiles_of(tokens, 128)
    for start in range(0, tokens, rows):
        query = jnp.dot(x_ref[start : start + rows, :], wq_ref[...], preferred_element_type=F32).astype(BF)
        for pair in range(heads // 2):
            proj = query[:, pair * 2 * dim_head : (pair + 1) * 2 * dim_head]
            feat_ref[start : start + rows, pair * 2 * nfeat : (pair + 1) * 2 * nfeat] = feature_tile(
                proj, pair_ref[pair], ones_ref[...], dim_head, nfeat
            )


def conv_kernel_body(top_ref, own_ref, low_ref, wv_ref, taps_ref, out_ref, ext_ref):
    here, cols, width = own_ref.shape
    ext_ref[1 : here + 1] = own_ref[...]
    ext_ref[0] = jnp.dot(top_ref[...], wv_ref[...], preferred_element_type=F32).astype(BF)
    ext_ref[here + 1] = jnp.dot(low_ref[...], wv_ref[...], preferred_element_type=F32).astype(BF)
    lanes = 128
    col = lax.broadcasted_iota(jnp.int32, (cols, lanes), 0)
    for start in range(0, width, lanes):
        cut = slice(start, start + lanes)
        for row in range(here):
            sums = []
            for shift in range(3):
                total = None
                for step in range(3):
                    term = ext_ref[row + step, :, cut].astype(F32) * taps_ref[step, shift : shift + 1, cut]
                    total = term if total is None else total + term
                sums.append(total)
            left = jnp.where(col == 0, 0.0, pltpu.roll(sums[0], 1, 0))
            right = jnp.where(col == cols - 1, 0.0, pltpu.roll(sums[2], cols - 1, 0))
            out_ref[row, :, cut] = left + sums[1] + right


def out_kernel(flip_ref, state_ref, feat_ref, pos_ref, x_ref, gain_ref, wo_ref, out_ref, mat_ref, attn_ref, *, heads):
    tokens, width = x_ref.shape
    dim_head = width // heads
    nfeat = state_ref.shape[-1]
    half = heads // 2
    wide = 2 * dim_head
    mat_ref[...] = jnp.zeros_like(mat_ref)
    for head in range(heads):
        pair, side = head // 2, head % 2
        slot = lax.rem(flip_ref[0] + head // half, 2)
        place = head % half
        cut = slice(side * nfeat, (side + 1) * nfeat)
        mat_ref[pair, side * dim_head : (side + 1) * dim_head, cut] = state_ref[slot, place * dim_head : (place + 1) * dim_head, :]
        sums = state_ref[slot, half * dim_head :, :][place : place + 1]
        mat_ref[pair, wide + side * dim_head : wide + (side + 1) * dim_head, cut] = jnp.broadcast_to(sums, (dim_head, nfeat))
    rows = tiles_of(tokens, 256)
    for start in range(0, tokens, rows):
        total = None
        for pair in range(heads // 2):
            both = lax.dot_general(
                feat_ref[start : start + rows, pair * 2 * nfeat : (pair + 1) * 2 * nfeat],
                mat_ref[pair],
                (((1,), (1,)), ((), ())),
                preferred_element_type=F32,
            )
            attn = both[:, :wide] / both[:, wide:]
            attn_ref[:, pair * wide : (pair + 1) * wide] = attn
            total = attn * attn if total is None else total + attn * attn
        scale = lax.rsqrt(jnp.sum(total, axis=1, keepdims=True) * (1.0 / width) + 1e-06)
        mixed = (attn_ref[...] * scale * gain_ref[...] + pos_ref[start : start + rows, :]).astype(BF)
        out = x_ref[start : start + rows, :].astype(F32) + jnp.dot(mixed, wo_ref[...], preferred_element_type=F32)
        out_ref[start : start + rows, :] = out.astype(BF)


def call(kernel, out_shape, n_in, scratch, smem=True, flops=0, nbytes=0):
    specs = ([pl.BlockSpec(memory_space=pltpu.SMEM)] if smem else []) + vmem_specs(n_in)
    many = isinstance(out_shape, (tuple, list))
    return pl.pallas_call(
        kernel,
        out_shape=out_shape,
        in_specs=specs,
        out_specs=vmem_specs(len(out_shape)) if many else vmem_specs(1)[0],
        scratch_shapes=scratch,
        compiler_params=pltpu.CompilerParams(vmem_limit_bytes=VMEM_LIMIT),
        cost_estimate=pl.CostEstimate(flops=flops, bytes_accessed=nbytes, transcendentals=0),
    )


def swap(block, bit, count, keep):
    return lax.ppermute(block, "row", [(i, i ^ bit) for i in range(count) if keep(i)])


def reduce_state(state, count):
    odd = lambda i: i % 2 == 1
    core = lax.rem(lax.axis_index("row"), 2)
    chip = state.astype(F32) + swap(state, 1, count, lambda i: i % 2 == 0).astype(F32)
    part = chip[0] + swap(chip[1].astype(BF), 2, count, odd).astype(F32)
    bit = 4
    while bit < count:
        part = part + swap(part.astype(BF), bit, count, odd).astype(F32)
        bit *= 2
    done = part.astype(BF)
    whole = jnp.stack([done, swap(done, 2, count, odd)])
    return jnp.where(core == 1, whole, swap(whole, 1, count, odd))


def shards(tokens, w_query, w_key, w_value, w_out, omega, conv_kernel, norm_gain):
    here, cols, width = tokens.shape
    heads, dim_head, nfeat = omega.shape
    count = lax.axis_size("row")
    flat = tokens.reshape(here * cols, width)
    amount = here * cols
    half = heads // 2
    flip = lax.rem(lax.axis_index("row") // 2, 2).astype(jnp.int32).reshape(1)
    proj = 2 * amount * width * width
    feats = 2 * amount * width * nfeat
    pairs = [pltpu.VMEM((heads // 2, 2 * dim_head, 2 * nfeat), BF), pltpu.VMEM((4 * dim_head, 4 * dim_head), BF)]

    top = lax.ppermute(tokens[here - 1], "row", [(i, i + 1) for i in range(count - 1)])
    low = lax.ppermute(tokens[0], "row", [(i + 1, i) for i in range(count - 1)])

    state, value = call(
        state_kernel,
        (
            jax.ShapeDtypeStruct((2, half * dim_head + 16, nfeat), BF),
            jax.ShapeDtypeStruct((amount, width), BF),
        ),
        4,
        pairs + [pltpu.VMEM((heads, dim_head + 16, amount), BF), pltpu.VMEM((amount, 2 * nfeat), BF)],
        flops=2 * proj + 2 * feats,
    )(flip, flat, w_key, w_value, omega)
    feat_query = call(
        query_kernel,
        jax.ShapeDtypeStruct((amount, heads * nfeat), BF),
        3,
        pairs,
        smem=False,
        flops=proj + feats,
    )(flat, w_query, omega)
    position = call(
        conv_kernel_body,
        jax.ShapeDtypeStruct((here, cols, width), F32),
        5,
        [pltpu.VMEM((here + 2, cols, width), BF)],
        smem=False,
        flops=proj,
    )(top, value.reshape(here, cols, width), low, w_value, conv_kernel)
    final = reduce_state(state, count)
    out = call(
        functools.partial(out_kernel, heads=heads),
        jax.ShapeDtypeStruct((amount, width), BF),
        6,
        [pltpu.VMEM((heads // 2, 4 * dim_head, 2 * nfeat), BF), pltpu.VMEM((tiles_of(amount, 256), width), F32)],
        flops=proj + 2 * feats,
    )(flip, final, feat_query, position.reshape(amount, width), flat, norm_gain.reshape(1, width), w_out)
    return out.reshape(here, cols, width)


def solution(mesh):
    return jax.shard_map(
        shards,
        mesh=mesh,
        in_specs=(P(("parts", "row"), None, None), P(), P(), P(), P(), P(), P(), P()),
        out_specs=P(("parts", "row"), None, None),
        check_vma=False,
    )
```

```python
import functools
import math

import jax
import jax.numpy as jnp
from jax import lax
from jax.experimental import pallas as pl
from jax.experimental.pallas import tpu as pltpu
from jax.sharding import PartitionSpec as P


BF = jnp.bfloat16
F32 = jnp.float32
LOG2E = 1.4426950408889634
VMEM_LIMIT = 28 * 1024 * 1024
VMEM_ALL = 67043328


def tiles_of(total, wanted):
    return wanted if total % wanted == 0 else total


def lift_scale(dim_head):
    return dim_head ** (-0.25) * LOG2E


def square_lanes(proj, dim_head, nfeat):
    quarter = dim_head // 2
    wide = 2 * dim_head
    scale = lift_scale(dim_head)
    values = proj.astype(F32)
    square = values * values * (0.5 * dim_head ** (-0.5) * LOG2E / scale)
    both = square + pltpu.roll(square, wide - quarter, 1)
    both = both + 0.5 * math.log2(nfeat) / scale / quarter
    high = both.astype(BF).astype(F32)
    low = both - high
    lane = lax.broadcasted_iota(jnp.int32, both.shape, 1)
    return jnp.where(lane % dim_head < quarter, high, pltpu.roll(low, quarter, 1)).astype(BF)


def feature_tile(proj, pair_mat, dim_head, nfeat):
    both = jnp.concatenate([proj, square_lanes(proj, dim_head, nfeat)], axis=1)
    lifted = jnp.dot(both, pair_mat, preferred_element_type=F32)
    return jnp.exp2(lifted * lift_scale(dim_head)).astype(BF)


def fill_pairs(omega_ref, pair_ref):
    heads, dim_head, nfeat = omega_ref.shape
    wide = 2 * dim_head
    empty = jnp.zeros((dim_head, nfeat), BF)
    minus = jnp.full((dim_head, nfeat), -1.0, BF)
    for head in range(heads):
        side = head % 2
        mine, other = slice(side * nfeat, (side + 1) * nfeat), slice((1 - side) * nfeat, (2 - side) * nfeat)
        for base, block in ((0, omega_ref[head]), (wide, minus)):
            rows = slice(base + side * dim_head, base + (side + 1) * dim_head)
            pair_ref[head // 2, rows, mine] = block
            pair_ref[head // 2, rows, other] = empty


def state_kernel(place_ref, x_hbm, wk_hbm, wv_hbm, omega_hbm, *refs):
    heads, dim_head, nfeat = omega_hbm.shape
    tokens, _ = x_hbm.shape
    here = len(refs) - 9
    state_ref, value_refs = refs[0], refs[1 : 1 + here]
    x_ref, wk_ref, wv_ref, omega_ref, sems, pair_ref, vt_ref, feat_ref = refs[1 + here :]
    copies = [
        pltpu.make_async_copy(source, target, sems.at[i])
        for i, (source, target) in enumerate(((x_hbm, x_ref), (wv_hbm, wv_ref), (omega_hbm, omega_ref), (wk_hbm, wk_ref)))
    ]
    for copy in copies:
        copy.start()
    group = heads // 4
    mark = lax.broadcasted_iota(jnp.int32, (16, tokens), 0)
    for head in range(heads):
        vt_ref[head, dim_head:, :] = jnp.where(mark == head % group, 1.0, 0.0).astype(BF)
    copies[0].wait()
    copies[1].wait()
    x = x_ref[...]
    value = jnp.dot(x, wv_ref[...], preferred_element_type=F32).astype(BF)
    cols = tokens // here
    for row in range(here):
        value_refs[row][...] = value[row * cols : (row + 1) * cols]
    turned = value.T
    for head in range(heads):
        vt_ref[head, :dim_head, :] = turned[head * dim_head : (head + 1) * dim_head]
    copies[2].wait()
    fill_pairs(omega_ref, pair_ref)
    copies[3].wait()
    rows = tiles_of(tokens, 128)
    sums = None
    for first in range(0, heads, 4):
        count = min(4, heads - first)
        key = jnp.dot(x, wk_ref[:, first * dim_head : (first + count) * dim_head], preferred_element_type=F32).astype(BF)
        for pair in range(count // 2):
            which = first // 2 + pair
            for start in range(0, tokens, rows):
                proj = key[start : start + rows, pair * 2 * dim_head : (pair + 1) * 2 * dim_head]
                feat_ref[start : start + rows, :] = feature_tile(proj, pair_ref[which], dim_head, nfeat)
            for side in range(2):
                head = 2 * which + side
                local = jnp.dot(vt_ref[head], feat_ref[:, side * nfeat : (side + 1) * nfeat], preferred_element_type=F32)
                owner = head // group
                slot = 2 * lax.rem(place_ref[0] + owner // 2, 2) + lax.rem(place_ref[1] + owner % 2, 2)
                spot = head % group
                state_ref[slot, spot * dim_head : (spot + 1) * dim_head, :] = local[:dim_head].astype(BF)
                sums = local[dim_head:] if spot == 0 else sums + local[dim_head:]
                if spot == group - 1:
                    state_ref[slot, group * dim_head :, :] = sums.astype(BF)


def query_kernel(x_ref, wq_ref, omega_ref, feat_ref, pair_ref):
    heads, dim_head, nfeat = omega_ref.shape
    tokens = x_ref.shape[0]
    fill_pairs(omega_ref, pair_ref)
    rows = tiles_of(tokens, 128)
    for start in range(0, tokens, rows):
        query = jnp.dot(x_ref[start : start + rows, :], wq_ref[...], preferred_element_type=F32).astype(BF)
        for pair in range(heads // 2):
            proj = query[:, pair * 2 * dim_head : (pair + 1) * 2 * dim_head]
            feat_ref[start : start + rows, pair * 2 * nfeat : (pair + 1) * 2 * nfeat] = feature_tile(
                proj, pair_ref[pair], dim_head, nfeat
            )


def conv_kernel_body(*refs):
    taps_ref, out_ref = refs[-2:]
    values = refs[:-2]
    here, cols, width = out_ref.shape
    lanes = 128
    col = lax.broadcasted_iota(jnp.int32, (cols, lanes), 0)
    for start in range(0, width, lanes):
        cut = slice(start, start + lanes)
        wide = [value[:, cut].astype(F32) for value in values]
        for row in range(here):
            sums = []
            for shift in range(3):
                terms = [wide[row + step] * taps_ref[step, shift : shift + 1, cut] for step in range(3)]
                sums.append(terms[0] + terms[1] + terms[2])
            left = jnp.where(col == 0, 0.0, pltpu.roll(sums[0], 1, 0))
            right = jnp.where(col == cols - 1, 0.0, pltpu.roll(sums[2], cols - 1, 0))
            out_ref[row, :, cut] = left + sums[1] + right


def out_kernel(place_ref, state_ref, feat_ref, pos_ref, x_ref, gain_ref, wo_ref, out_ref, mat_ref, attn_ref, *, heads):
    tokens, width = x_ref.shape
    dim_head = width // heads
    nfeat = state_ref.shape[-1]
    group = heads // 4
    wide = 2 * dim_head
    mat_ref[...] = jnp.zeros_like(mat_ref)
    for head in range(heads):
        pair, side = head // 2, head % 2
        owner = head // group
        slot = 2 * lax.rem(place_ref[0] + owner // 2, 2) + lax.rem(place_ref[1] + owner % 2, 2)
        place = head % group
        cut = slice(side * nfeat, (side + 1) * nfeat)
        mat_ref[pair, side * dim_head : (side + 1) * dim_head, cut] = state_ref[slot, place * dim_head : (place + 1) * dim_head, :]
        sums = state_ref[slot, group * dim_head :, :][place : place + 1]
        mat_ref[pair, wide + side * dim_head : wide + (side + 1) * dim_head, cut] = jnp.broadcast_to(sums, (dim_head, nfeat))
    rows = tiles_of(tokens, 256)
    for start in range(0, tokens, rows):
        total = None
        for pair in range(heads // 2):
            both = lax.dot_general(
                feat_ref[start : start + rows, pair * 2 * nfeat : (pair + 1) * 2 * nfeat],
                mat_ref[pair],
                (((1,), (1,)), ((), ())),
                preferred_element_type=F32,
            )
            attn = both[:, :wide] / both[:, wide:]
            attn_ref[:, pair * wide : (pair + 1) * wide] = attn
            total = attn * attn if total is None else total + attn * attn
        scale = lax.rsqrt(jnp.sum(total, axis=1, keepdims=True) * (1.0 / width) + 1e-06)
        mixed = (attn_ref[...] * scale * gain_ref[...] + pos_ref[start : start + rows, :]).astype(BF)
        out = x_ref[start : start + rows, :].astype(F32) + jnp.dot(mixed, wo_ref[...], preferred_element_type=F32)
        out_ref[start : start + rows, :] = out.astype(BF)


def call(kernel, out_shape, in_specs, scratch, flops, limit=VMEM_LIMIT):
    out_specs = [pl.BlockSpec(memory_space=pltpu.VMEM)] * len(out_shape)
    return pl.pallas_call(
        kernel,
        out_shape=out_shape,
        in_specs=in_specs,
        out_specs=out_specs,
        scratch_shapes=scratch,
        compiler_params=pltpu.CompilerParams(vmem_limit_bytes=limit),
        cost_estimate=pl.CostEstimate(flops=flops, bytes_accessed=0, transcendentals=0),
    )


def swap(block, bit, count):
    return lax.ppermute(block, "row", [(i, i ^ bit) for i in range(count)])


def reduce_state(state, count):
    other = swap(state[2:], 1, count)
    chip = state[:2].astype(F32) + other.astype(F32)
    other = swap(chip[1].astype(BF), 2, count)
    part = chip[0] + other.astype(F32)
    bit = 4
    while bit < count:
        other = swap(part.astype(BF), bit, count)
        part = part + other.astype(F32)
        bit *= 2
    done = part.astype(BF)
    other = swap(done, 2, count)
    half = jnp.stack([done, other])
    other = swap(half, 1, count)
    return jnp.concatenate([half, other])


def layer(tokens, w_query, w_key, w_value, w_out, omega, conv_kernel, norm_gain):
    here, cols, width = tokens.shape
    heads, dim_head, nfeat = omega.shape
    count = lax.axis_size("row")
    flat = tokens.reshape(here * cols, width)
    amount = here * cols
    group = heads // 4
    spot = lax.axis_index("row").astype(jnp.int32)
    place = jnp.stack([lax.bitwise_and(spot, 1), lax.bitwise_and(lax.shift_right_logical(spot, 1), 1)])
    proj = 2 * amount * width * width
    feats = 2 * amount * width * nfeat
    pairs = pltpu.VMEM((heads // 2, 4 * dim_head, 2 * nfeat), BF)
    vmem = pl.BlockSpec(memory_space=pltpu.VMEM)
    smem = pl.BlockSpec(memory_space=pltpu.SMEM)
    hbm = pl.BlockSpec(memory_space=pltpu.HBM)

    state, *values = call(
        state_kernel,
        [jax.ShapeDtypeStruct((4, group * dim_head + 16, nfeat), BF)] + [jax.ShapeDtypeStruct((cols, width), BF)] * here,
        [smem] + [hbm] * 4,
        [
            pltpu.VMEM((amount, width), BF),
            pltpu.VMEM((width, width), BF),
            pltpu.VMEM((width, width), BF),
            pltpu.VMEM((heads, dim_head, nfeat), BF),
            pltpu.SemaphoreType.DMA((4,)),
            pairs,
            pltpu.VMEM((heads, dim_head + 16, amount), BF),
            pltpu.VMEM((amount, 2 * nfeat), BF),
        ],
        2 * proj + 2 * feats,
        VMEM_ALL - 2 * (amount * width + 4 * (group * dim_head + 16) * nfeat) - 10400000,
    )(place, flat, w_key, w_value, omega)
    top = lax.ppermute(values[-1], "row", [(i, i + 1) for i in range(count - 1)])
    low = lax.ppermute(values[0], "row", [(i + 1, i) for i in range(count - 1)])
    (feat_query,) = call(
        query_kernel, [jax.ShapeDtypeStruct((amount, heads * nfeat), BF)], [vmem] * 3, [pairs], proj + feats
    )(flat, w_query, omega)
    (position,) = call(
        conv_kernel_body, [jax.ShapeDtypeStruct((here, cols, width), F32)], [vmem] * (here + 3), [], proj
    )(top, *values, low, conv_kernel)
    final = reduce_state(state, count)
    (out,) = call(
        functools.partial(out_kernel, heads=heads),
        [jax.ShapeDtypeStruct((amount, width), BF)],
        [smem] + [vmem] * 6,
        [pltpu.VMEM((heads // 2, 4 * dim_head, 2 * nfeat), BF), pltpu.VMEM((tiles_of(amount, 256), width), F32)],
        proj + 2 * feats,
    )(place, final, feat_query, position.reshape(amount, width), flat, norm_gain.reshape(1, width), w_out)
    return out.reshape(here, cols, width)


def solution(mesh):
    return jax.shard_map(
        layer,
        mesh=mesh,
        in_specs=(P(("parts", "row"), None, None), P(), P(), P(), P(), P(), P(), P()),
        out_specs=P(("parts", "row"), None, None),
        check_vma=False,
    )
```

```python
import math

import jax
import jax.numpy as jnp
from jax import lax
from jax.experimental import pallas as pl
from jax.experimental.pallas import tpu as pltpu
from jax.sharding import PartitionSpec as P


BF = jnp.bfloat16
F32 = jnp.float32
LOG2E = 1.4426950408889634
VMEM_LIMIT = 28 * 1024 * 1024
FIRST_LIMIT = 54500000


def tiles_of(total, wanted):
    return wanted if total % wanted == 0 else total


def feature_tile(proj, omega_pair, ones_pair, dim_head, nfeat):
    wide = 2 * dim_head
    lifted = jnp.dot(proj, omega_pair, preferred_element_type=F32)
    values = proj.astype(F32)
    square = values * values * (0.5 * dim_head ** (-0.5) * LOG2E)
    high = square.astype(BF)
    low = (square - high.astype(F32)).astype(BF)
    summed = jnp.dot(jnp.concatenate([high, low], axis=1), ones_pair, preferred_element_type=F32)
    parts = []
    for head in range(2):
        drop = summed[:, head * wide : (head + 1) * wide] + 0.5 * math.log2(nfeat)
        for part in range(nfeat // wide):
            start = head * nfeat + part * wide
            grown = lifted[:, start : start + wide] * (dim_head ** (-0.25) * LOG2E)
            parts.append(jnp.exp2(grown - drop).astype(BF))
    return jnp.concatenate(parts, axis=1)


def fill_pair(pair_ref, which, omegas):
    dim_head, nfeat = omegas[0].shape
    empty = jnp.zeros((dim_head, nfeat), BF)
    for side in range(2):
        rows = slice(side * dim_head, (side + 1) * dim_head)
        pair_ref[which, rows, side * nfeat : (side + 1) * nfeat] = omegas[side]
        pair_ref[which, rows, (1 - side) * nfeat : (2 - side) * nfeat] = empty


def fill_ones(ones_ref, dim_head):
    row = lax.broadcasted_iota(jnp.int32, ones_ref.shape, 0) // dim_head % 2
    col = lax.broadcasted_iota(jnp.int32, ones_ref.shape, 1) // (2 * dim_head)
    ones_ref[...] = jnp.where(row == col, 1.0, 0.0).astype(BF)


def fill_marks(vt_ref, group):
    heads, rows, tokens = vt_ref.shape
    mark = lax.broadcasted_iota(jnp.int32, (16, tokens), 0)
    for head in range(heads):
        vt_ref[head, rows - 16 :, :] = jnp.where(mark == head % group, 1.0, 0.0).astype(BF)


def half_state(bit, key, pair_ref, ones_ref, vt_ref, feat_ref, state_ref):
    heads, rows, tokens = vt_ref.shape
    dim_head = rows - 16
    nfeat = feat_ref.shape[1] // 2
    group = heads // 2
    tile = tiles_of(tokens, 128)
    sums = None
    for head in range(heads):
        pair, side = head // 2, head % 2
        if side == 0:
            for start in range(0, tokens, tile):
                proj = key[start : start + tile, pair * 2 * dim_head : (pair + 1) * 2 * dim_head]
                feat_ref[start : start + tile, :] = feature_tile(proj, pair_ref[pair], ones_ref[...], dim_head, nfeat)
        local = jnp.dot(vt_ref[head], feat_ref[:, side * nfeat : (side + 1) * nfeat], preferred_element_type=F32)
        slot = lax.rem(bit + head // group, 2)
        spot = head % group
        state_ref[slot, spot * dim_head : (spot + 1) * dim_head, :] = local[:dim_head].astype(state_ref.dtype)
        sums = local[dim_head:] if spot == 0 else sums + local[dim_head:]
        if spot == group - 1:
            state_ref[slot, group * dim_head :, :] = sums.astype(state_ref.dtype)


def first_kernel(place_ref, x_hbm, wk_hbm, wv_hbm, omega_hbm, *refs):
    heads, dim_head, _ = omega_hbm.shape
    tokens, width = x_hbm.shape
    here = len(refs) - 12
    send_ref, key_ref, own_ref = refs[:3]
    value_refs = refs[3 : 3 + here]
    x_ref, wk_ref, wv_ref, omega_ref, sems, pair_ref, ones_ref, vt_ref, feat_ref = refs[3 + here :]
    half, span = heads // 2, width // 2
    core = place_ref[0]
    sides = [pl.multiple_of((1 - core) * span, span), pl.multiple_of(core * span, span)]
    moves = [(x_hbm, x_ref)]
    moves += [(wv_hbm.at[:, pl.ds(side, span)], wv_ref.at[i]) for i, side in enumerate(sides)]
    moves += [(omega_hbm.at[pl.ds((1 - core) * half, half)], omega_ref)]
    moves += [(wk_hbm.at[:, pl.ds(side, span)], wk_ref.at[i]) for i, side in enumerate(sides)]
    copies = [pltpu.make_async_copy(source, target, sems.at[i]) for i, (source, target) in enumerate(moves)]
    for copy in copies:
        copy.start()
    fill_ones(ones_ref, dim_head)
    fill_marks(vt_ref, half // 2)
    copies[0].wait()
    x = x_ref[...]
    cols = tokens // here
    for i in range(2):
        copies[1 + i].wait()
        value = jnp.dot(x, wv_ref[i], preferred_element_type=F32).astype(BF)
        for row in range(here):
            value_refs[row][:, pl.ds(sides[i], span)] = value[row * cols : (row + 1) * cols]
        if i == 0:
            turned = value.T
            for head in range(half):
                vt_ref[head, :dim_head, :] = turned[head * dim_head : (head + 1) * dim_head]
        else:
            own_ref[...] = value
    copies[3].wait()
    for pair in range(half // 2):
        fill_pair(pair_ref, pair, [omega_ref[2 * pair], omega_ref[2 * pair + 1]])
    copies[4].wait()
    key = jnp.dot(x, wk_ref[0], preferred_element_type=F32).astype(BF)
    half_state(place_ref[1], key, pair_ref, ones_ref, vt_ref, feat_ref, send_ref)
    copies[5].wait()
    key_ref[...] = jnp.dot(x, wk_ref[1], preferred_element_type=F32).astype(BF)


def second_kernel(place_ref, key_ref, own_ref, omega_ref, state_ref, pair_ref, ones_ref, vt_ref, feat_ref):
    heads, dim_head, _ = omega_ref.shape
    half = heads // 2
    base = place_ref[0] * half
    fill_ones(ones_ref, dim_head)
    fill_marks(vt_ref, half // 2)
    turned = own_ref[...].T
    for head in range(half):
        vt_ref[head, :dim_head, :] = turned[head * dim_head : (head + 1) * dim_head]
    for pair in range(half // 2):
        fill_pair(pair_ref, pair, [omega_ref[base + 2 * pair], omega_ref[base + 2 * pair + 1]])
    half_state(place_ref[1], key_ref, pair_ref, ones_ref, vt_ref, feat_ref, state_ref)


def query_kernel(place_ref, x_ref, wq_ref, omega_ref, own_ref, other_ref, pair_ref, ones_ref):
    heads, dim_head, nfeat = omega_ref.shape
    tokens, width = x_ref.shape
    half, span = heads // 2, width // 2
    fill_ones(ones_ref, dim_head)
    tile = tiles_of(tokens, 128)
    for i, feat_ref in enumerate((own_ref, other_ref)):
        part = lax.rem(place_ref[0] + i, 2)
        weight = wq_ref[:, pl.ds(pl.multiple_of(part * span, span), span)]
        for pair in range(half // 2):
            head = part * half + 2 * pair
            fill_pair(pair_ref, i * (half // 2) + pair, [omega_ref[head], omega_ref[head + 1]])
        for start in range(0, tokens, tile):
            query = jnp.dot(x_ref[start : start + tile, :], weight, preferred_element_type=F32).astype(BF)
            for pair in range(half // 2):
                proj = query[:, pair * 2 * dim_head : (pair + 1) * 2 * dim_head]
                feat_ref[start : start + tile, pair * 2 * nfeat : (pair + 1) * 2 * nfeat] = feature_tile(
                    proj, pair_ref[i * (half // 2) + pair], ones_ref[...], dim_head, nfeat
                )


def conv_kernel_body(*refs):
    taps_ref, out_ref = refs[-2:]
    values = refs[:-2]
    here, cols, width = out_ref.shape
    lanes = 128
    col = lax.broadcasted_iota(jnp.int32, (cols, lanes), 0)
    for start in range(0, width, lanes):
        cut = slice(start, start + lanes)
        wide = [value[:, cut].astype(F32) for value in values]
        for row in range(here):
            sums = []
            for shift in range(3):
                terms = [wide[row + step] * taps_ref[step, shift : shift + 1, cut] for step in range(3)]
                sums.append(terms[0] + terms[1] + terms[2])
            left = jnp.where(col == 0, 0.0, pltpu.roll(sums[0], 1, 0))
            right = jnp.where(col == cols - 1, 0.0, pltpu.roll(sums[2], cols - 1, 0))
            out_ref[row, :, cut] = left + sums[1] + right


def fill_mats(bit, state_ref, mat_ref, dim_head):
    pairs, _, both = mat_ref.shape
    nfeat = both // 2
    group = pairs
    wide = 2 * dim_head
    empty = jnp.zeros((dim_head, nfeat), BF)
    for head in range(2 * pairs):
        pair, side = head // 2, head % 2
        slot = lax.rem(bit + head // group, 2)
        spot = head % group
        mine, other = slice(side * nfeat, (side + 1) * nfeat), slice((1 - side) * nfeat, (2 - side) * nfeat)
        sums = state_ref[slot, group * dim_head :, :][spot : spot + 1]
        for base, block in (
            (0, state_ref[slot, spot * dim_head : (spot + 1) * dim_head, :]),
            (wide, jnp.broadcast_to(sums, (dim_head, nfeat))),
        ):
            rows = slice(base + side * dim_head, base + (side + 1) * dim_head)
            mat_ref[pair, rows, mine] = block
            mat_ref[pair, rows, other] = empty


def attend(feat, mat, wide):
    both = lax.dot_general(feat, mat, (((1,), (1,)), ((), ())), preferred_element_type=F32)
    return both[:, :wide] / both[:, wide:]


def own_kernel(place_ref, state_ref, feat_ref, attn_ref, mat_ref):
    pairs, rows, both = mat_ref.shape
    wide = rows // 2
    tokens = attn_ref.shape[0]
    fill_mats(place_ref[1], state_ref, mat_ref, wide // 2)
    tile = tiles_of(tokens, 256)
    for start in range(0, tokens, tile):
        for pair in range(pairs):
            attn_ref[start : start + tile, pair * wide : (pair + 1) * wide] = attend(
                feat_ref[start : start + tile, pair * both : (pair + 1) * both], mat_ref[pair], wide
            )


def out_kernel(place_ref, state_ref, feat_ref, own_ref, pos_ref, x_ref, gain_ref, wo_ref, out_ref, mat_ref, attn_ref):
    pairs, rows, both = mat_ref.shape
    wide = rows // 2
    tokens, width = x_ref.shape
    span = width // 2
    core = place_ref[0]
    fill_mats(place_ref[1], state_ref, mat_ref, wide // 2)
    mine = pl.ds(pl.multiple_of(core * span, span), span)
    other = pl.ds(pl.multiple_of((1 - core) * span, span), span)
    tile = tiles_of(tokens, 256)
    for start in range(0, tokens, tile):
        cut = slice(start, start + tile)
        total = None
        for pair in range(pairs):
            lanes = slice(pair * wide, (pair + 1) * wide)
            attn = attend(feat_ref[cut, pair * both : (pair + 1) * both], mat_ref[pair], wide)
            attn_ref[:, lanes] = attn
            kept = own_ref[cut, lanes]
            square = attn * attn + kept * kept
            total = square if total is None else total + square
        scale = lax.rsqrt(jnp.sum(total, axis=1, keepdims=True) * (1.0 / width) + 1e-06)
        out = x_ref[cut, :].astype(F32)
        for part, attn in ((mine, own_ref[cut, :]), (other, attn_ref[...])):
            mixed = (attn * scale * gain_ref[:, part] + pos_ref[cut, part]).astype(BF)
            out = out + jnp.dot(mixed, wo_ref[part, :], preferred_element_type=F32)
        out_ref[cut, :] = out.astype(BF)


def call(kernel, out_shape, in_specs, scratch, flops, limit=VMEM_LIMIT):
    return pl.pallas_call(
        kernel,
        out_shape=out_shape,
        in_specs=in_specs,
        out_specs=[pl.BlockSpec(memory_space=pltpu.VMEM)] * len(out_shape),
        scratch_shapes=scratch,
        compiler_params=pltpu.CompilerParams(vmem_limit_bytes=limit),
        cost_estimate=pl.CostEstimate(flops=flops, bytes_accessed=0, transcendentals=0),
    )


def swap(block, bit, count):
    return lax.ppermute(block, "row", [(i, i ^ bit) for i in range(count)])


def reduce_half(send, keep, count, split):
    other = swap(send, 1, count)
    chip = keep + other.astype(F32)
    other = swap(chip[1].astype(BF), split, count)
    part = chip[0] + other.astype(F32)
    bit = count // 2
    while bit > 1:
        if bit != split:
            other = swap(part.astype(BF), bit, count)
            part = part + other.astype(F32)
        bit //= 2
    done = part.astype(BF)
    other = swap(done, split, count)
    return jnp.stack([done, other])


def layer(tokens, w_query, w_key, w_value, w_out, omega, conv_kernel, norm_gain):
    here, cols, width = tokens.shape
    heads, dim_head, nfeat = omega.shape
    count = lax.axis_size("row")
    split = min(4, count // 2)
    flat = tokens.reshape(here * cols, width)
    amount = here * cols
    half, span = heads // 2, width // 2
    rows = half // 2 * dim_head + 16
    spot = lax.axis_index("row").astype(jnp.int32)
    place = jnp.stack([lax.bitwise_and(spot, 1), lax.bitwise_and(lax.shift_right_logical(spot, split.bit_length() - 1), 1)])
    proj = 2 * amount * width * width
    feats = 2 * amount * width * nfeat
    vmem = pl.BlockSpec(memory_space=pltpu.VMEM)
    smem = pl.BlockSpec(memory_space=pltpu.SMEM)
    hbm = pl.BlockSpec(memory_space=pltpu.HBM)
    pairs = pltpu.VMEM((half // 2, 2 * dim_head, 2 * nfeat), BF)
    ones = pltpu.VMEM((4 * dim_head, 4 * dim_head), BF)
    turned = pltpu.VMEM((half, dim_head + 16, amount), BF)
    feat = pltpu.VMEM((amount, 2 * nfeat), BF)
    mats = pltpu.VMEM((half // 2, 4 * dim_head, 2 * nfeat), BF)

    send, key, own, *values = call(
        first_kernel,
        [
            jax.ShapeDtypeStruct((2, rows, nfeat), BF),
            jax.ShapeDtypeStruct((amount, span), BF),
            jax.ShapeDtypeStruct((amount, span), BF),
        ]
        + [jax.ShapeDtypeStruct((cols, width), BF)] * here,
        [smem] + [hbm] * 4,
        [
            pltpu.VMEM((amount, width), BF),
            pltpu.VMEM((2, width, span), BF),
            pltpu.VMEM((2, width, span), BF),
            pltpu.VMEM((half, dim_head, nfeat), BF),
            pltpu.SemaphoreType.DMA((6,)),
            pairs,
            ones,
            turned,
            feat,
        ],
        2 * proj + feats,
        FIRST_LIMIT,
    )(place, flat, w_key, w_value, omega)
    (keep,) = call(
        second_kernel,
        [jax.ShapeDtypeStruct((2, rows, nfeat), F32)],
        [smem] + [vmem] * 3,
        [pairs, ones, turned, feat],
        feats,
    )(place, key, own, omega)
    top = lax.ppermute(values[-1], "row", [(i, i + 1) for i in range(count - 1)])
    low = lax.ppermute(values[0], "row", [(i + 1, i) for i in range(count - 1)])
    feat_own, feat_other = call(
        query_kernel,
        [jax.ShapeDtypeStruct((amount, half * nfeat), BF)] * 2,
        [smem] + [vmem] * 3,
        [pltpu.VMEM((half, 2 * dim_head, 2 * nfeat), BF), ones],
        proj + feats,
    )(place, flat, w_query, omega)
    (position,) = call(
        conv_kernel_body, [jax.ShapeDtypeStruct((here, cols, width), F32)], [vmem] * (here + 3), [], proj
    )(top, *values, low, conv_kernel)
    mine = reduce_half(send, keep, count, split)
    theirs = swap(mine, 1, count)
    (attn,) = call(
        own_kernel, [jax.ShapeDtypeStruct((amount, span), F32)], [smem] + [vmem] * 2, [mats], feats
    )(place, mine, feat_own)
    (out,) = call(
        out_kernel,
        [jax.ShapeDtypeStruct((amount, width), BF)],
        [smem] + [vmem] * 7,
        [mats, pltpu.VMEM((tiles_of(amount, 256), span), F32)],
        proj + feats,
    )(place, theirs, feat_other, attn, position.reshape(amount, width), flat, norm_gain.reshape(1, width), w_out)
    return out.reshape(here, cols, width)


def solution(mesh):
    return jax.shard_map(
        layer,
        mesh=mesh,
        in_specs=(P(("parts", "row"), None, None), P(), P(), P(), P(), P(), P(), P()),
        out_specs=P(("parts", "row"), None, None),
        check_vma=False,
    )
```

```python
import functools
import math

import jax
import jax.numpy as jnp
from jax import lax
from jax.experimental import pallas as pl
from jax.experimental.pallas import tpu as pltpu
from jax.sharding import PartitionSpec as P


BF = jnp.bfloat16
F32 = jnp.float32
LOG2E = 1.4426950408889634
TILE = 256
VMEM_LIMIT = 28 * 1024 * 1024
FIRST_LIMIT = 54900000


def tiles_of(total, wanted):
    return wanted if total % wanted == 0 else total


def feature_tile(proj, omega_pair, dim_head, nfeat):
    lifted = jnp.dot(proj, omega_pair, preferred_element_type=F32)
    values = proj.astype(F32)
    square = values * values * (0.5 * dim_head ** (-0.5) * LOG2E)
    first = lax.broadcasted_iota(jnp.int32, square.shape, 1) < dim_head
    halves = []
    for head, mine in enumerate((jnp.where(first, square, 0.0), jnp.where(first, 0.0, square))):
        drop = jnp.sum(mine, axis=1, keepdims=True) + 0.5 * math.log2(nfeat)
        grown = lifted[:, head * nfeat : (head + 1) * nfeat] * (dim_head ** (-0.25) * LOG2E)
        halves.append(jnp.exp2(grown - drop).astype(BF))
    return jnp.concatenate(halves, axis=1)


def fill_pair(pair_ref, which, omegas):
    dim_head, nfeat = omegas[0].shape
    empty = jnp.zeros((dim_head, nfeat), BF)
    for side in range(2):
        rows = slice(side * dim_head, (side + 1) * dim_head)
        pair_ref[which, rows, side * nfeat : (side + 1) * nfeat] = omegas[side]
        pair_ref[which, rows, (1 - side) * nfeat : (2 - side) * nfeat] = empty


def fill_marks(vt_ref, group):
    heads, rows, tokens = vt_ref.shape
    mark = lax.broadcasted_iota(jnp.int32, (16, tokens), 0)
    for head in range(heads):
        vt_ref[head, rows - 16 :, :] = jnp.where(mark == head % group, 1.0, 0.0).astype(BF)


def half_state(bit, key_ref, offset, pair_ref, vt_ref, feat_ref, state_ref):
    heads, rows, tokens = vt_ref.shape
    dim_head = rows - 16
    wide = 2 * dim_head
    nfeat = feat_ref.shape[1] // 2
    group = heads // 2
    tile = tiles_of(tokens, TILE)
    sums = None
    for head in range(heads):
        pair, side = head // 2, head % 2
        if side == 0:
            lanes = slice(pair * wide, (pair + 1) * wide) if isinstance(offset, int) else pl.ds(pl.multiple_of(offset + pair * wide, wide), wide)
            for start in range(0, tokens, tile):
                feat_ref[start : start + tile, :] = feature_tile(key_ref[start : start + tile, lanes], pair_ref[pair], dim_head, nfeat)
        local = jnp.dot(vt_ref[head], feat_ref[:, side * nfeat : (side + 1) * nfeat], preferred_element_type=F32)
        slot = lax.rem(bit + head // group, 2)
        spot = head % group
        state_ref[slot, spot * dim_head : (spot + 1) * dim_head, :] = local[:dim_head].astype(state_ref.dtype)
        sums = local[dim_head:] if spot == 0 else sums + local[dim_head:]
        if spot == group - 1:
            state_ref[slot, group * dim_head :, :] = sums.astype(state_ref.dtype)


def turn_values(value_refs, offset, span, vt_ref):
    heads, rows, _ = vt_ref.shape
    dim_head = rows - 16
    lanes = pl.ds(pl.multiple_of(offset, span), span)
    turned = jnp.concatenate([ref[:, lanes] for ref in value_refs], axis=0).T
    for head in range(heads):
        vt_ref[head, :dim_head, :] = turned[head * dim_head : (head + 1) * dim_head]


def first_kernel(place_ref, x_hbm, wk_hbm, wv_hbm, omega_hbm, *refs):
    heads, _, _ = omega_hbm.shape
    tokens, width = x_hbm.shape
    here = len(refs) - 11
    send_ref, own_ref = refs[:2]
    value_refs = refs[2 : 2 + here]
    x_ref, wk_ref, wv_ref, omega_ref, key_ref, sems, pair_ref, vt_ref, feat_ref = refs[2 + here :]
    half, span = heads // 2, width // 2
    other = 1 - place_ref[0]
    moves = [(x_hbm, x_ref), (wv_hbm, wv_ref), (omega_hbm.at[pl.ds(other * half, half)], omega_ref), (wk_hbm, wk_ref)]
    copies = [pltpu.make_async_copy(source, target, sems.at[i]) for i, (source, target) in enumerate(moves)]
    for copy in copies:
        copy.start()
    fill_marks(vt_ref, half // 2)
    cols = tokens // here
    blocks = [slice(row * cols, (row + 1) * cols) for row in range(here)]
    copies[0].wait()
    copies[1].wait()
    for block, value_ref in zip(blocks, value_refs):
        value_ref[...] = jnp.dot(x_ref[block, :], wv_ref[...], preferred_element_type=F32).astype(BF)
    copies[2].wait()
    for pair in range(half // 2):
        fill_pair(pair_ref, pair, [omega_ref[2 * pair], omega_ref[2 * pair + 1]])
    copies[3].wait()
    for block in blocks:
        key_ref[block, :] = jnp.dot(x_ref[block, :], wk_ref[...], preferred_element_type=F32).astype(BF)
    own_ref[...] = key_ref[:, pl.ds(pl.multiple_of(place_ref[0] * span, span), span)]
    turn_values(value_refs, other * span, span, vt_ref)
    half_state(place_ref[1], key_ref, other * span, pair_ref, vt_ref, feat_ref, send_ref)


def second_kernel(place_ref, key_ref, omega_ref, *refs):
    heads, _, _ = omega_ref.shape
    value_refs = refs[:-4]
    state_ref, pair_ref, vt_ref, feat_ref = refs[-4:]
    half, span = heads // 2, key_ref.shape[1]
    core = place_ref[0]
    fill_marks(vt_ref, half // 2)
    for pair in range(half // 2):
        fill_pair(pair_ref, pair, [omega_ref[core * half + 2 * pair], omega_ref[core * half + 2 * pair + 1]])
    turn_values(value_refs, core * span, span, vt_ref)
    half_state(place_ref[1], key_ref, 0, pair_ref, vt_ref, feat_ref, state_ref)


def query_kernel(x_ref, wq_ref, omega_ref, feat_ref, pair_ref):
    heads, dim_head, nfeat = omega_ref.shape
    tokens = x_ref.shape[0]
    for pair in range(heads // 2):
        fill_pair(pair_ref, pair, [omega_ref[2 * pair], omega_ref[2 * pair + 1]])
    tile = tiles_of(tokens, TILE)
    for start in range(0, tokens, tile):
        query = jnp.dot(x_ref[start : start + tile, :], wq_ref[...], preferred_element_type=F32).astype(BF)
        for pair in range(heads // 2):
            proj = query[:, pair * 2 * dim_head : (pair + 1) * 2 * dim_head]
            feat_ref[start : start + tile, pair * 2 * nfeat : (pair + 1) * 2 * nfeat] = feature_tile(
                proj, pair_ref[pair], dim_head, nfeat
            )


def conv_kernel_body(*refs):
    taps_ref, out_ref = refs[-2:]
    values = refs[:-2]
    here, cols, width = out_ref.shape
    lanes = 128
    col = lax.broadcasted_iota(jnp.int32, (cols, lanes), 0)
    for start in range(0, width, lanes):
        cut = slice(start, start + lanes)
        wide = [value[:, cut].astype(F32) for value in values]
        for row in range(here):
            sums = []
            for shift in range(3):
                terms = [wide[row + step] * taps_ref[step, shift : shift + 1, cut] for step in range(3)]
                sums.append(terms[0] + terms[1] + terms[2])
            left = jnp.where(col == 0, 0.0, pltpu.roll(sums[0], 1, 0))
            right = jnp.where(col == cols - 1, 0.0, pltpu.roll(sums[2], cols - 1, 0))
            out_ref[row, :, cut] = left + sums[1] + right


def fill_mats(bit, state_ref, mat_ref, dim_head):
    pairs, _, both = mat_ref.shape
    nfeat = both // 2
    group = pairs
    wide = 2 * dim_head
    empty = jnp.zeros((dim_head, nfeat), BF)
    for head in range(2 * pairs):
        pair, side = head // 2, head % 2
        slot = lax.rem(bit + head // group, 2)
        spot = head % group
        mine, other = slice(side * nfeat, (side + 1) * nfeat), slice((1 - side) * nfeat, (2 - side) * nfeat)
        sums = state_ref[slot, group * dim_head :, :][spot : spot + 1]
        for base, block in (
            (0, state_ref[slot, spot * dim_head : (spot + 1) * dim_head, :]),
            (wide, jnp.broadcast_to(sums, (dim_head, nfeat))),
        ):
            rows = slice(base + side * dim_head, base + (side + 1) * dim_head)
            mat_ref[pair, rows, mine] = block
            mat_ref[pair, rows, other] = empty


def attend(feat, mat, wide):
    both = lax.dot_general(feat, mat, (((1,), (1,)), ((), ())), preferred_element_type=F32)
    return both[:, :wide] / both[:, wide:]


def own_kernel(place_ref, state_ref, feat_ref, attn_ref, mat_ref):
    pairs, rows, both = mat_ref.shape
    wide = rows // 2
    tokens = attn_ref.shape[0]
    fill_mats(place_ref[1], state_ref, mat_ref, wide // 2)
    tile = tiles_of(tokens, 256)
    for start in range(0, tokens, tile):
        for pair in range(pairs):
            attn_ref[start : start + tile, pair * wide : (pair + 1) * wide] = attend(
                feat_ref[start : start + tile, pl.ds(pl.multiple_of((place_ref[0] * pairs + pair) * both, both), both)], mat_ref[pair], wide
            )


def out_kernel(place_ref, state_ref, feat_ref, own_ref, pos_ref, x_ref, gain_ref, wo_ref, out_ref, mat_ref, attn_ref):
    pairs, rows, both = mat_ref.shape
    wide = rows // 2
    tokens, width = x_ref.shape
    span = width // 2
    core = place_ref[0]
    fill_mats(place_ref[1], state_ref, mat_ref, wide // 2)
    mine = pl.ds(pl.multiple_of(core * span, span), span)
    other = pl.ds(pl.multiple_of((1 - core) * span, span), span)
    tile = tiles_of(tokens, 256)
    for start in range(0, tokens, tile):
        cut = slice(start, start + tile)
        total = None
        for pair in range(pairs):
            lanes = slice(pair * wide, (pair + 1) * wide)
            attn = attend(feat_ref[cut, pl.ds(pl.multiple_of(((1 - core) * pairs + pair) * both, both), both)], mat_ref[pair], wide)
            attn_ref[:, lanes] = attn
            kept = own_ref[cut, lanes]
            square = attn * attn + kept * kept
            total = square if total is None else total + square
        scale = lax.rsqrt(jnp.sum(total, axis=1, keepdims=True) * (1.0 / width) + 1e-06)
        out = x_ref[cut, :].astype(F32)
        for part, attn in ((mine, own_ref[cut, :]), (other, attn_ref[...])):
            mixed = (attn * scale * gain_ref[:, part] + pos_ref[cut, part]).astype(BF)
            out = out + jnp.dot(mixed, wo_ref[part, :], preferred_element_type=F32)
        out_ref[cut, :] = out.astype(BF)


def call(kernel, out_shape, in_specs, scratch, flops, limit=VMEM_LIMIT):
    return pl.pallas_call(
        kernel,
        out_shape=out_shape,
        in_specs=in_specs,
        out_specs=[pl.BlockSpec(memory_space=pltpu.VMEM)] * len(out_shape),
        scratch_shapes=scratch,
        compiler_params=pltpu.CompilerParams(vmem_limit_bytes=limit),
        cost_estimate=pl.CostEstimate(flops=flops, bytes_accessed=0, transcendentals=0),
    )


def swap(block, bit, count):
    return lax.ppermute(block, "row", [(i, i ^ bit ^ (bit > 1)) for i in range(count)])


def reduce_half(send, keep, count, split):
    other = swap(send, 1, count)
    chip = keep + other.astype(F32)
    other = swap(chip[1].astype(BF), split, count)
    part = chip[0] + other.astype(F32)
    bit = count // 2
    while bit > 1:
        if bit != split:
            other = swap(part.astype(BF), bit, count)
            part = part + other.astype(F32)
        bit //= 2
    done = part.astype(BF)
    other = swap(done, split, count)
    return jnp.stack([done, other])


def layer(tokens, w_query, w_key, w_value, w_out, omega, conv_kernel, norm_gain):
    here, cols, width = tokens.shape
    heads, dim_head, nfeat = omega.shape
    count = lax.axis_size("row")
    split = min(4, count // 2)
    flat = tokens.reshape(here * cols, width)
    amount = here * cols
    half, span = heads // 2, width // 2
    rows = half // 2 * dim_head + 16
    spot = lax.axis_index("row").astype(jnp.int32)
    bits = [lax.bitwise_and(lax.shift_right_logical(spot, i), 1) for i in range(count.bit_length() - 1)]
    place = jnp.stack([functools.reduce(lax.bitwise_xor, bits), bits[split.bit_length() - 1]])
    proj = 2 * amount * width * width
    feats = 2 * amount * width * nfeat
    vmem = pl.BlockSpec(memory_space=pltpu.VMEM)
    smem = pl.BlockSpec(memory_space=pltpu.SMEM)
    hbm = pl.BlockSpec(memory_space=pltpu.HBM)
    pairs = pltpu.VMEM((half // 2, 2 * dim_head, 2 * nfeat), BF)
    turned = pltpu.VMEM((half, dim_head + 16, amount), BF)
    feat = pltpu.VMEM((amount, 2 * nfeat), BF)
    mats = pltpu.VMEM((half // 2, 4 * dim_head, 2 * nfeat), BF)

    send, key, *values = call(
        first_kernel,
        [jax.ShapeDtypeStruct((2, rows, nfeat), BF), jax.ShapeDtypeStruct((amount, span), BF)]
        + [jax.ShapeDtypeStruct((cols, width), BF)] * here,
        [smem] + [hbm] * 4,
        [
            pltpu.VMEM((amount, width), BF),
            pltpu.VMEM((width, width), BF),
            pltpu.VMEM((width, width), BF),
            pltpu.VMEM((half, dim_head, nfeat), BF),
            pltpu.VMEM((amount, width), BF),
            pltpu.SemaphoreType.DMA((4,)),
            pairs,
            turned,
            feat,
        ],
        2 * proj + feats,
        FIRST_LIMIT,
    )(place, flat, w_key, w_value, omega)
    (keep,) = call(
        second_kernel,
        [jax.ShapeDtypeStruct((2, rows, nfeat), F32)],
        [smem] + [vmem] * (2 + here),
        [pairs, turned, feat],
        feats,
    )(place, key, omega, *values)
    top = lax.ppermute(values[-1], "row", [(i, i + 1) for i in range(count - 1)])
    low = lax.ppermute(values[0], "row", [(i + 1, i) for i in range(count - 1)])
    (feat_query,) = call(
        query_kernel,
        [jax.ShapeDtypeStruct((amount, heads * nfeat), BF)],
        [vmem] * 3,
        [pltpu.VMEM((half, 2 * dim_head, 2 * nfeat), BF)],
        proj + feats,
    )(flat, w_query, omega)
    (position,) = call(
        conv_kernel_body, [jax.ShapeDtypeStruct((here, cols, width), F32)], [vmem] * (here + 3), [], proj
    )(top, *values, low, conv_kernel)
    mine = reduce_half(send, keep, count, split)
    theirs = swap(mine, 1, count)
    (attn,) = call(
        own_kernel, [jax.ShapeDtypeStruct((amount, span), F32)], [smem] + [vmem] * 2, [mats], feats
    )(place, mine, feat_query)
    (out,) = call(
        out_kernel,
        [jax.ShapeDtypeStruct((amount, width), BF)],
        [smem] + [vmem] * 7,
        [mats, pltpu.VMEM((tiles_of(amount, 256), span), F32)],
        proj + feats,
    )(place, theirs, feat_query, attn, position.reshape(amount, width), flat, norm_gain.reshape(1, width), w_out)
    return out.reshape(here, cols, width)


def solution(mesh):
    return jax.shard_map(
        layer,
        mesh=mesh,
        in_specs=(P(("parts", "row"), None, None), P(), P(), P(), P(), P(), P(), P()),
        out_specs=P(("parts", "row"), None, None),
        check_vma=False,
    )
```

```python
import functools
import math

import jax
import jax.numpy as jnp
from jax import lax
from jax.experimental import pallas as pl
from jax.experimental.pallas import tpu as pltpu
from jax.sharding import PartitionSpec as P


BF = jnp.bfloat16
F32 = jnp.float32
LOG2E = 1.4426950408889634
TILE = 256
VMEM_LIMIT = 28 * 1024 * 1024
FIRST_LIMIT = 54900000


def tiles_of(total, wanted):
    return wanted if total % wanted == 0 else total


def feature_tile(proj, omega_pair, dim_head, nfeat):
    lifted = jnp.dot(proj, omega_pair, preferred_element_type=F32)
    values = proj.astype(F32)
    square = values * values * (0.5 * dim_head ** (-0.5) * LOG2E)
    first = lax.broadcasted_iota(jnp.int32, square.shape, 1) < dim_head
    halves = []
    for head, mine in enumerate((jnp.where(first, square, 0.0), jnp.where(first, 0.0, square))):
        drop = jnp.sum(mine, axis=1, keepdims=True) + 0.5 * math.log2(nfeat)
        grown = lifted[:, head * nfeat : (head + 1) * nfeat] * (dim_head ** (-0.25) * LOG2E)
        halves.append(jnp.exp2(grown - drop).astype(BF))
    return jnp.concatenate(halves, axis=1)


def fill_pair(pair_ref, which, omegas):
    dim_head, nfeat = omegas[0].shape
    empty = jnp.zeros((dim_head, nfeat), BF)
    for side in range(2):
        rows = slice(side * dim_head, (side + 1) * dim_head)
        pair_ref[which, rows, side * nfeat : (side + 1) * nfeat] = omegas[side]
        pair_ref[which, rows, (1 - side) * nfeat : (2 - side) * nfeat] = empty


def fill_marks(vt_ref, group):
    heads, rows, tokens = vt_ref.shape
    mark = lax.broadcasted_iota(jnp.int32, (16, tokens), 0)
    for head in range(heads):
        vt_ref[head, rows - 16 :, :] = jnp.where(mark == head % group, 1.0, 0.0).astype(BF)


def half_state(bit, key_ref, offset, pair_ref, vt_ref, feat_ref, state_ref):
    heads, rows, tokens = vt_ref.shape
    dim_head = rows - 16
    wide = 2 * dim_head
    nfeat = feat_ref.shape[1] // 2
    group = heads // 2
    tile = tiles_of(tokens, TILE)
    sums = None
    for head in range(heads):
        pair, side = head // 2, head % 2
        if side == 0:
            lanes = slice(pair * wide, (pair + 1) * wide) if isinstance(offset, int) else pl.ds(pl.multiple_of(offset + pair * wide, wide), wide)
            for start in range(0, tokens, tile):
                feat_ref[start : start + tile, :] = feature_tile(key_ref[start : start + tile, lanes], pair_ref[pair], dim_head, nfeat)
        local = jnp.dot(vt_ref[head], feat_ref[:, side * nfeat : (side + 1) * nfeat], preferred_element_type=F32)
        slot = lax.rem(bit + head // group, 2)
        spot = head % group
        state_ref[slot, spot * dim_head : (spot + 1) * dim_head, :] = local[:dim_head].astype(state_ref.dtype)
        sums = local[dim_head:] if spot == 0 else sums + local[dim_head:]
        if spot == group - 1:
            state_ref[slot, group * dim_head :, :] = sums.astype(state_ref.dtype)


def turn_values(value_refs, offset, span, vt_ref):
    heads, rows, _ = vt_ref.shape
    dim_head = rows - 16
    lanes = pl.ds(pl.multiple_of(offset, span), span)
    turned = jnp.concatenate([ref[:, lanes] for ref in value_refs], axis=0).T
    for head in range(heads):
        vt_ref[head, :dim_head, :] = turned[head * dim_head : (head + 1) * dim_head]


def first_kernel(place_ref, x_hbm, wk_hbm, wv_hbm, omega_hbm, *refs):
    heads, _, _ = omega_hbm.shape
    tokens, width = x_hbm.shape
    here = len(refs) - 11
    send_ref, own_ref = refs[:2]
    value_refs = refs[2 : 2 + here]
    x_ref, wk_ref, wv_ref, omega_ref, key_ref, sems, pair_ref, vt_ref, feat_ref = refs[2 + here :]
    half, span = heads // 2, width // 2
    other = 1 - place_ref[0]
    moves = [(x_hbm, x_ref), (wv_hbm, wv_ref), (omega_hbm.at[pl.ds(other * half, half)], omega_ref), (wk_hbm, wk_ref)]
    copies = [pltpu.make_async_copy(source, target, sems.at[i]) for i, (source, target) in enumerate(moves)]
    for copy in copies:
        copy.start()
    fill_marks(vt_ref, half // 2)
    cols = tokens // here
    turn = 1 - place_ref[2]
    blocks = [pl.ds(pl.multiple_of((row + turn * (here - 1 - 2 * row)) * cols, cols), cols) for row in range(here)]
    copies[0].wait()
    copies[1].wait()
    for block, value_ref in zip(blocks, value_refs):
        value_ref[...] = jnp.dot(x_ref[block, :], wv_ref[...], preferred_element_type=F32).astype(BF)
    copies[2].wait()
    for pair in range(half // 2):
        fill_pair(pair_ref, pair, [omega_ref[2 * pair], omega_ref[2 * pair + 1]])
    copies[3].wait()
    for row, block in enumerate(blocks):
        key_ref[row * cols : (row + 1) * cols, :] = jnp.dot(x_ref[block, :], wk_ref[...], preferred_element_type=F32).astype(BF)
    own_ref[...] = key_ref[:, pl.ds(pl.multiple_of(place_ref[0] * span, span), span)]
    turn_values(value_refs, other * span, span, vt_ref)
    half_state(place_ref[1], key_ref, other * span, pair_ref, vt_ref, feat_ref, send_ref)


def second_kernel(place_ref, key_ref, omega_ref, *refs):
    heads, _, _ = omega_ref.shape
    value_refs = refs[:-4]
    state_ref, pair_ref, vt_ref, feat_ref = refs[-4:]
    half, span = heads // 2, key_ref.shape[1]
    core = place_ref[0]
    fill_marks(vt_ref, half // 2)
    for pair in range(half // 2):
        fill_pair(pair_ref, pair, [omega_ref[core * half + 2 * pair], omega_ref[core * half + 2 * pair + 1]])
    turn_values(value_refs, core * span, span, vt_ref)
    half_state(place_ref[1], key_ref, 0, pair_ref, vt_ref, feat_ref, state_ref)


def query_kernel(x_ref, wq_ref, omega_ref, feat_ref, pair_ref):
    heads, dim_head, nfeat = omega_ref.shape
    tokens = x_ref.shape[0]
    for pair in range(heads // 2):
        fill_pair(pair_ref, pair, [omega_ref[2 * pair], omega_ref[2 * pair + 1]])
    tile = tiles_of(tokens, TILE)
    for start in range(0, tokens, tile):
        query = jnp.dot(x_ref[start : start + tile, :], wq_ref[...], preferred_element_type=F32).astype(BF)
        for pair in range(heads // 2):
            proj = query[:, pair * 2 * dim_head : (pair + 1) * 2 * dim_head]
            feat_ref[start : start + tile, pair * 2 * nfeat : (pair + 1) * 2 * nfeat] = feature_tile(
                proj, pair_ref[pair], dim_head, nfeat
            )


def conv_kernel_body(place_ref, *refs):
    taps_ref, out_ref = refs[-2:]
    values = refs[:-2]
    here, cols, width = out_ref.shape
    turn = 1 - place_ref[2]
    lanes = 128
    col = lax.broadcasted_iota(jnp.int32, (cols, lanes), 0)
    for start in range(0, width, lanes):
        cut = slice(start, start + lanes)
        wide = [value[:, cut].astype(F32) for value in values]
        taps = [taps_ref[step + turn * (2 - 2 * step), :, cut] for step in range(3)]
        for row in range(here):
            sums = []
            for shift in range(3):
                terms = [wide[row + step] * taps[step][shift : shift + 1] for step in range(3)]
                sums.append(terms[0] + terms[1] + terms[2])
            left = jnp.where(col == 0, 0.0, pltpu.roll(sums[0], 1, 0))
            right = jnp.where(col == cols - 1, 0.0, pltpu.roll(sums[2], cols - 1, 0))
            out_ref[row + turn * (here - 1 - 2 * row), :, cut] = left + sums[1] + right


def fill_mats(bit, state_ref, mat_ref, dim_head):
    pairs, _, both = mat_ref.shape
    nfeat = both // 2
    group = pairs
    wide = 2 * dim_head
    empty = jnp.zeros((dim_head, nfeat), BF)
    for head in range(2 * pairs):
        pair, side = head // 2, head % 2
        slot = lax.rem(bit + head // group, 2)
        spot = head % group
        mine, other = slice(side * nfeat, (side + 1) * nfeat), slice((1 - side) * nfeat, (2 - side) * nfeat)
        sums = state_ref[slot, group * dim_head :, :][spot : spot + 1]
        for base, block in (
            (0, state_ref[slot, spot * dim_head : (spot + 1) * dim_head, :]),
            (wide, jnp.broadcast_to(sums, (dim_head, nfeat))),
        ):
            rows = slice(base + side * dim_head, base + (side + 1) * dim_head)
            mat_ref[pair, rows, mine] = block
            mat_ref[pair, rows, other] = empty


def attend(feat, mat, wide):
    both = lax.dot_general(feat, mat, (((1,), (1,)), ((), ())), preferred_element_type=F32)
    return both[:, :wide] / both[:, wide:]


def own_kernel(place_ref, state_ref, feat_ref, attn_ref, mat_ref):
    pairs, rows, both = mat_ref.shape
    wide = rows // 2
    tokens = attn_ref.shape[0]
    fill_mats(place_ref[1], state_ref, mat_ref, wide // 2)
    tile = tiles_of(tokens, 256)
    for start in range(0, tokens, tile):
        for pair in range(pairs):
            attn_ref[start : start + tile, pair * wide : (pair + 1) * wide] = attend(
                feat_ref[start : start + tile, pl.ds(pl.multiple_of((place_ref[0] * pairs + pair) * both, both), both)], mat_ref[pair], wide
            )


def out_kernel(place_ref, state_ref, feat_ref, own_ref, pos_ref, x_ref, gain_ref, wo_ref, out_ref, mat_ref, attn_ref):
    pairs, rows, both = mat_ref.shape
    wide = rows // 2
    tokens, width = x_ref.shape
    span = width // 2
    core = place_ref[0]
    fill_mats(place_ref[1], state_ref, mat_ref, wide // 2)
    mine = pl.ds(pl.multiple_of(core * span, span), span)
    other = pl.ds(pl.multiple_of((1 - core) * span, span), span)
    tile = tiles_of(tokens, 256)
    for start in range(0, tokens, tile):
        cut = slice(start, start + tile)
        total = None
        for pair in range(pairs):
            lanes = slice(pair * wide, (pair + 1) * wide)
            attn = attend(feat_ref[cut, pl.ds(pl.multiple_of(((1 - core) * pairs + pair) * both, both), both)], mat_ref[pair], wide)
            attn_ref[:, lanes] = attn
            kept = own_ref[cut, lanes]
            square = attn * attn + kept * kept
            total = square if total is None else total + square
        scale = lax.rsqrt(jnp.sum(total, axis=1, keepdims=True) * (1.0 / width) + 1e-06)
        out = x_ref[cut, :].astype(F32)
        for part, attn in ((mine, own_ref[cut, :]), (other, attn_ref[...])):
            mixed = (attn * scale * gain_ref[:, part] + pos_ref[cut, part]).astype(BF)
            out = out + jnp.dot(mixed, wo_ref[part, :], preferred_element_type=F32)
        out_ref[cut, :] = out.astype(BF)


def call(kernel, out_shape, in_specs, scratch, flops, limit=VMEM_LIMIT):
    return pl.pallas_call(
        kernel,
        out_shape=out_shape,
        in_specs=in_specs,
        out_specs=[pl.BlockSpec(memory_space=pltpu.VMEM)] * len(out_shape),
        scratch_shapes=scratch,
        compiler_params=pltpu.CompilerParams(vmem_limit_bytes=limit),
        cost_estimate=pl.CostEstimate(flops=flops, bytes_accessed=0, transcendentals=0),
    )


def swap(block, bit, count):
    return lax.ppermute(block, "row", [(i, i ^ bit ^ (bit > 1)) for i in range(count)])


def reduce_half(send, keep, count, split):
    other = swap(send, 1, count)
    chip = keep + other.astype(F32)
    other = swap(chip[1].astype(BF), split, count)
    part = chip[0] + other.astype(F32)
    bit = count // 2
    while bit > 1:
        if bit != split:
            other = swap(part.astype(BF), bit, count)
            part = part + other.astype(F32)
        bit //= 2
    done = part.astype(BF)
    other = swap(done, split, count)
    return jnp.stack([done, other])


def layer(tokens, w_query, w_key, w_value, w_out, omega, conv_kernel, norm_gain):
    here, cols, width = tokens.shape
    heads, dim_head, nfeat = omega.shape
    count = lax.axis_size("row")
    split = min(4, count // 2)
    flat = tokens.reshape(here * cols, width)
    amount = here * cols
    half, span = heads // 2, width // 2
    rows = half // 2 * dim_head + 16
    spot = lax.axis_index("row").astype(jnp.int32)
    bits = [lax.bitwise_and(lax.shift_right_logical(spot, i), 1) for i in range(count.bit_length() - 1)]
    place = jnp.stack([functools.reduce(lax.bitwise_xor, bits), bits[split.bit_length() - 1], bits[0]])
    proj = 2 * amount * width * width
    feats = 2 * amount * width * nfeat
    vmem = pl.BlockSpec(memory_space=pltpu.VMEM)
    smem = pl.BlockSpec(memory_space=pltpu.SMEM)
    hbm = pl.BlockSpec(memory_space=pltpu.HBM)
    pairs = pltpu.VMEM((half // 2, 2 * dim_head, 2 * nfeat), BF)
    turned = pltpu.VMEM((half, dim_head + 16, amount), BF)
    feat = pltpu.VMEM((amount, 2 * nfeat), BF)
    mats = pltpu.VMEM((half // 2, 4 * dim_head, 2 * nfeat), BF)

    send, key, *values = call(
        first_kernel,
        [jax.ShapeDtypeStruct((2, rows, nfeat), BF), jax.ShapeDtypeStruct((amount, span), BF)]
        + [jax.ShapeDtypeStruct((cols, width), BF)] * here,
        [smem] + [hbm] * 4,
        [
            pltpu.VMEM((amount, width), BF),
            pltpu.VMEM((width, width), BF),
            pltpu.VMEM((width, width), BF),
            pltpu.VMEM((half, dim_head, nfeat), BF),
            pltpu.VMEM((amount, width), BF),
            pltpu.SemaphoreType.DMA((4,)),
            pairs,
            turned,
            feat,
        ],
        2 * proj + feats,
        FIRST_LIMIT,
    )(place, flat, w_key, w_value, omega)
    (keep,) = call(
        second_kernel,
        [jax.ShapeDtypeStruct((2, rows, nfeat), F32)],
        [smem] + [vmem] * (2 + here),
        [pairs, turned, feat],
        feats,
    )(place, key, omega, *values)
    near = swap(values[0], 1, count)
    gaps = [(i, i + 1) for i in range(1, count - 1, 2)]
    far = lax.ppermute(values[-1], "row", gaps + [(high, low) for low, high in gaps])
    (feat_query,) = call(
        query_kernel,
        [jax.ShapeDtypeStruct((amount, heads * nfeat), BF)],
        [vmem] * 3,
        [pltpu.VMEM((half, 2 * dim_head, 2 * nfeat), BF)],
        proj + feats,
    )(flat, w_query, omega)
    (position,) = call(
        conv_kernel_body, [jax.ShapeDtypeStruct((here, cols, width), F32)], [smem] + [vmem] * (here + 3), [], proj
    )(place, near, *values, far, conv_kernel)
    mine = reduce_half(send, keep, count, split)
    theirs = swap(mine, 1, count)
    (attn,) = call(
        own_kernel, [jax.ShapeDtypeStruct((amount, span), F32)], [smem] + [vmem] * 2, [mats], feats
    )(place, mine, feat_query)
    (out,) = call(
        out_kernel,
        [jax.ShapeDtypeStruct((amount, width), BF)],
        [smem] + [vmem] * 7,
        [mats, pltpu.VMEM((tiles_of(amount, 256), span), F32)],
        proj + feats,
    )(place, theirs, feat_query, attn, position.reshape(amount, width), flat, norm_gain.reshape(1, width), w_out)
    return out.reshape(here, cols, width)


def solution(mesh):
    return jax.shard_map(
        layer,
        mesh=mesh,
        in_specs=(P(("parts", "row"), None, None), P(), P(), P(), P(), P(), P(), P()),
        out_specs=P(("parts", "row"), None, None),
        check_vma=False,
    )
```

```python
import math

import jax
import jax.numpy as jnp
from jax import lax
from jax.experimental import pallas as pl
from jax.experimental.pallas import tpu as pltpu
from jax.sharding import PartitionSpec as P


BF = jnp.bfloat16
F32 = jnp.float32
LOG2E = 1.4426950408889634
TILE = 256
VMEM_LIMIT = 28 * 1024 * 1024
FIRST_LIMIT = 54900000


def tiles_of(total, wanted):
    return wanted if total % wanted == 0 else total


def feature_tile(proj, omega_pair, dim_head, nfeat):
    lifted = jnp.dot(proj, omega_pair, preferred_element_type=F32)
    values = proj.astype(F32)
    square = values * values * (0.5 * dim_head ** (-0.5) * LOG2E)
    first = lax.broadcasted_iota(jnp.int32, square.shape, 1) < dim_head
    halves = []
    for head, mine in enumerate((jnp.where(first, square, 0.0), jnp.where(first, 0.0, square))):
        drop = jnp.sum(mine, axis=1, keepdims=True) + 0.5 * math.log2(nfeat)
        grown = lifted[:, head * nfeat : (head + 1) * nfeat] * (dim_head ** (-0.25) * LOG2E)
        halves.append(jnp.exp2(grown - drop).astype(BF))
    return jnp.concatenate(halves, axis=1)


def fill_pair(pair_ref, which, omegas):
    dim_head, nfeat = omegas[0].shape
    empty = jnp.zeros((dim_head, nfeat), BF)
    for side in range(2):
        rows = slice(side * dim_head, (side + 1) * dim_head)
        pair_ref[which, rows, side * nfeat : (side + 1) * nfeat] = omegas[side]
        pair_ref[which, rows, (1 - side) * nfeat : (2 - side) * nfeat] = empty


def fill_marks(vt_ref, group):
    heads, rows, tokens = vt_ref.shape
    mark = lax.broadcasted_iota(jnp.int32, (16, tokens), 0)
    for head in range(heads):
        vt_ref[head, rows - 16 :, :] = jnp.where(mark == head % group, 1.0, 0.0).astype(BF)


def half_state(bit, key_ref, offset, pair_ref, vt_ref, feat_ref, state_ref):
    heads, rows, tokens = vt_ref.shape
    dim_head = rows - 16
    wide = 2 * dim_head
    nfeat = feat_ref.shape[2] // 2
    group = heads // 2
    tile = tiles_of(tokens, TILE)
    sums = None
    for pair in range(heads // 2):
            lanes = slice(pair * wide, (pair + 1) * wide) if isinstance(offset, int) else pl.ds(pl.multiple_of(offset + pair * wide, wide), wide)
            for start in range(0, tokens, tile):
                feat_ref[pair, start : start + tile, :] = feature_tile(key_ref[start : start + tile, lanes], pair_ref[pair], dim_head, nfeat)
    for head in range(heads):
        pair, side = head // 2, head % 2
        local = jnp.dot(vt_ref[head], feat_ref[pair, :, side * nfeat : (side + 1) * nfeat], preferred_element_type=F32)
        slot = lax.rem(bit + head // group, 2)
        spot = head % group
        state_ref[slot, spot * dim_head : (spot + 1) * dim_head, :] = local[:dim_head].astype(state_ref.dtype)
        sums = local[dim_head:] if spot == 0 else sums + local[dim_head:]
        if spot == group - 1:
            state_ref[slot, group * dim_head :, :] = sums[:8].astype(state_ref.dtype)


def turn_values(value_refs, offset, span, vt_ref):
    heads, rows, _ = vt_ref.shape
    dim_head = rows - 16
    lanes = pl.ds(pl.multiple_of(offset, span), span)
    turned = jnp.concatenate([ref[:, lanes] for ref in value_refs], axis=0).T
    for head in range(heads):
        vt_ref[head, :dim_head, :] = turned[head * dim_head : (head + 1) * dim_head]


def first_kernel(place_ref, x_hbm, wk_hbm, wv_hbm, omega_hbm, *refs):
    heads, _, _ = omega_hbm.shape
    tokens, width = x_hbm.shape
    here = len(refs) - 11
    send_ref, own_ref = refs[:2]
    value_refs = refs[2 : 2 + here]
    x_ref, wk_ref, wv_ref, omega_ref, key_ref, sems, pair_ref, vt_ref, feat_ref = refs[2 + here :]
    half, span = heads // 2, width // 2
    other = 1 - place_ref[0]
    moves = [(x_hbm, x_ref), (wv_hbm, wv_ref), (omega_hbm.at[pl.ds(other * half, half)], omega_ref), (wk_hbm, wk_ref)]
    copies = [pltpu.make_async_copy(source, target, sems.at[i]) for i, (source, target) in enumerate(moves)]
    for copy in copies:
        copy.start()
    fill_marks(vt_ref, half // 2)
    cols = tokens // here
    blocks = [slice(row * cols, (row + 1) * cols) for row in range(here)]
    copies[0].wait()
    copies[1].wait()
    for block, value_ref in zip(blocks, value_refs):
        value_ref[...] = jnp.dot(x_ref[block, :], wv_ref[...], preferred_element_type=F32).astype(BF)
    copies[2].wait()
    for pair in range(half // 2):
        fill_pair(pair_ref, pair, [omega_ref[2 * pair], omega_ref[2 * pair + 1]])
    copies[3].wait()
    for block in blocks:
        key_ref[block, :] = jnp.dot(x_ref[block, :], wk_ref[...], preferred_element_type=F32).astype(BF)
    own_ref[...] = key_ref[:, pl.ds(pl.multiple_of(place_ref[0] * span, span), span)]
    turn_values(value_refs, other * span, span, vt_ref)
    half_state(place_ref[1], key_ref, other * span, pair_ref, vt_ref, feat_ref, send_ref)


def second_kernel(place_ref, key_ref, omega_ref, *refs):
    heads, _, _ = omega_ref.shape
    value_refs = refs[:-4]
    state_ref, pair_ref, vt_ref, feat_ref = refs[-4:]
    half, span = heads // 2, key_ref.shape[1]
    core = place_ref[0]
    fill_marks(vt_ref, half // 2)
    for pair in range(half // 2):
        fill_pair(pair_ref, pair, [omega_ref[core * half + 2 * pair], omega_ref[core * half + 2 * pair + 1]])
    turn_values(value_refs, core * span, span, vt_ref)
    half_state(place_ref[1], key_ref, 0, pair_ref, vt_ref, feat_ref, state_ref)


def query_kernel(x_ref, wq_ref, omega_ref, feat_ref, pair_ref):
    heads, dim_head, nfeat = omega_ref.shape
    tokens = x_ref.shape[0]
    for pair in range(heads // 2):
        fill_pair(pair_ref, pair, [omega_ref[2 * pair], omega_ref[2 * pair + 1]])
    tile = tiles_of(tokens, TILE)
    for start in range(0, tokens, tile):
        query = jnp.dot(x_ref[start : start + tile, :], wq_ref[...], preferred_element_type=F32).astype(BF)
        for pair in range(heads // 2):
            proj = query[:, pair * 2 * dim_head : (pair + 1) * 2 * dim_head]
            feat_ref[start : start + tile, pair * 2 * nfeat : (pair + 1) * 2 * nfeat] = feature_tile(
                proj, pair_ref[pair], dim_head, nfeat
            )


def conv_kernel_body(*refs):
    x_ref, wo_ref, taps_ref, out_ref, pos_ref = refs[-5:]
    values = refs[:-5]
    here = len(values) - 2
    cols, width = values[0].shape
    lanes = 128
    col = lax.broadcasted_iota(jnp.int32, (cols, lanes), 0)
    for start in range(0, width, lanes):
        cut = slice(start, start + lanes)
        wide = [value[:, cut].astype(F32) for value in values]
        for row in range(here):
            sums = []
            for shift in range(3):
                terms = [wide[row + step] * taps_ref[step, shift : shift + 1, cut] for step in range(3)]
                sums.append(terms[0] + terms[1] + terms[2])
            left = jnp.where(col == 0, 0.0, pltpu.roll(sums[0], 1, 0))
            right = jnp.where(col == cols - 1, 0.0, pltpu.roll(sums[2], cols - 1, 0))
            pos_ref[row * cols : (row + 1) * cols, cut] = (left + sums[1] + right).astype(BF)
    for row in range(here):
        cut = slice(row * cols, (row + 1) * cols)
        out_ref[cut, :] = x_ref[cut, :].astype(F32) + jnp.dot(pos_ref[cut, :], wo_ref[...], preferred_element_type=F32)


def fill_mats(bit, state_ref, mat_ref, dim_head):
    pairs, _, both = mat_ref.shape
    nfeat = both // 2
    group = pairs
    wide = 2 * dim_head
    empty = jnp.zeros((dim_head, nfeat), BF)
    for head in range(2 * pairs):
        pair, side = head // 2, head % 2
        slot = lax.rem(bit + head // group, 2)
        spot = head % group
        mine, other = slice(side * nfeat, (side + 1) * nfeat), slice((1 - side) * nfeat, (2 - side) * nfeat)
        sums = state_ref[slot, group * dim_head :, :][spot : spot + 1]
        for base, block in (
            (0, state_ref[slot, spot * dim_head : (spot + 1) * dim_head, :]),
            (wide, jnp.broadcast_to(sums, (dim_head, nfeat))),
        ):
            rows = slice(base + side * dim_head, base + (side + 1) * dim_head)
            mat_ref[pair, rows, mine] = block
            mat_ref[pair, rows, other] = empty


def attend(feat, mat, wide):
    both = lax.dot_general(feat, mat, (((1,), (1,)), ((), ())), preferred_element_type=F32)
    return both[:, :wide] / both[:, wide:]


def own_kernel(place_ref, state_ref, feat_ref, gain_ref, wo_ref, part_ref, square_ref, mat_ref):
    pairs, rows, _ = mat_ref.shape
    wide = rows // 2
    tokens = part_ref.shape[0]
    span = pairs * wide
    core = place_ref[0]
    fill_mats(place_ref[1], state_ref, mat_ref, wide // 2)
    tile = tiles_of(tokens, 256)
    for start in range(0, tokens, tile):
        cut = slice(start, start + tile)
        part_ref[cut, :], square_ref[cut, :] = half_share(core, span, feat_ref, cut, gain_ref, wo_ref, mat_ref)


def half_share(side, span, feat_ref, cut, gain_ref, wo_ref, mat_ref):
    pairs, rows, both = mat_ref.shape
    wide = rows // 2
    base = pl.multiple_of(side * span, span)
    total, scaled = None, []
    for pair in range(pairs):
        lanes = pl.ds(pl.multiple_of((side * pairs + pair) * both, both), both)
        attn = attend(feat_ref[cut, lanes], mat_ref[pair], wide)
        total = attn * attn if total is None else total + attn * attn
        gain = gain_ref[:, pl.ds(pl.multiple_of(base + pair * wide, wide), wide)]
        scaled.append((attn * gain).astype(BF))
    share = jnp.dot(jnp.concatenate(scaled, axis=1), wo_ref[pl.ds(base, span), :], preferred_element_type=F32)
    return share, total


def out_kernel(place_ref, state_ref, feat_ref, part_ref, square_ref, base_ref, gain_ref, wo_ref, out_hbm, mat_ref, out_ref, sems):
    _, rows, _ = mat_ref.shape
    wide = rows // 2
    tokens, width = base_ref.shape
    fill_mats(place_ref[1], state_ref, mat_ref, wide // 2)
    tile = tiles_of(tokens, 256)
    copies = []
    for start in range(0, tokens, tile):
        cut = slice(start, start + tile)
        share, total = half_share(1 - place_ref[0], width // 2, feat_ref, cut, gain_ref, wo_ref, mat_ref)
        total = total + square_ref[cut, :]
        scale = lax.rsqrt(jnp.sum(total, axis=1, keepdims=True) * (1.0 / width) + 1e-06)
        out_ref[cut, :] = (base_ref[cut, :] + scale * (share + part_ref[cut, :])).astype(BF)
        copies.append(pltpu.make_async_copy(out_ref.at[cut], out_hbm.at[cut], sems.at[start // tile]))
        copies[-1].start()
    for copy in copies:
        copy.wait()


def call(kernel, out_shape, in_specs, scratch, flops, limit=VMEM_LIMIT, space=pltpu.VMEM):
    return pl.pallas_call(
        kernel,
        out_shape=out_shape,
        in_specs=in_specs,
        out_specs=[pl.BlockSpec(memory_space=space)] * len(out_shape),
        scratch_shapes=scratch,
        compiler_params=pltpu.CompilerParams(vmem_limit_bytes=limit),
        cost_estimate=pl.CostEstimate(flops=flops, bytes_accessed=0, transcendentals=0),
    )


def swap(block, bit, count):
    return lax.ppermute(block, "row", [(i, i ^ bit) for i in range(count)])


def reduce_half(send, keep, count, split):
    other = swap(send, 1, count)
    chip = keep + other.astype(F32)
    other = swap(chip[1].astype(BF), split, count)
    part = chip[0] + other.astype(F32)
    bit = count // 2
    while bit > 1:
        if bit != split:
            other = swap(part.astype(BF), bit, count)
            part = part + other.astype(F32)
        bit //= 2
    done = part.astype(BF)
    other = swap(done, split, count)
    return jnp.stack([done, other])


def layer(tokens, w_query, w_key, w_value, w_out, omega, conv_kernel, norm_gain):
    here, cols, width = tokens.shape
    heads, dim_head, nfeat = omega.shape
    count = lax.axis_size("row")
    split = min(4, count // 2)
    flat = tokens.reshape(here * cols, width)
    amount = here * cols
    half, span = heads // 2, width // 2
    rows = half // 2 * dim_head + 8
    spot = lax.axis_index("row").astype(jnp.int32)
    bits = [lax.bitwise_and(lax.shift_right_logical(spot, i), 1) for i in range(count.bit_length() - 1)]
    place = jnp.stack([bits[0], bits[split.bit_length() - 1]])
    proj = 2 * amount * width * width
    feats = 2 * amount * width * nfeat
    vmem = pl.BlockSpec(memory_space=pltpu.VMEM)
    smem = pl.BlockSpec(memory_space=pltpu.SMEM)
    hbm = pl.BlockSpec(memory_space=pltpu.HBM)
    pairs = pltpu.VMEM((half // 2, 2 * dim_head, 2 * nfeat), BF)
    turned = pltpu.VMEM((half, dim_head + 16, amount), BF)
    feat = pltpu.VMEM((half // 2, amount, 2 * nfeat), BF)
    mats = pltpu.VMEM((half // 2, 4 * dim_head, 2 * nfeat), BF)

    send, key, *values = call(
        first_kernel,
        [jax.ShapeDtypeStruct((2, rows, nfeat), BF), jax.ShapeDtypeStruct((amount, span), BF)]
        + [jax.ShapeDtypeStruct((cols, width), BF)] * here,
        [smem] + [hbm] * 4,
        [
            pltpu.VMEM((amount, width), BF),
            pltpu.VMEM((width, width), BF),
            pltpu.VMEM((width, width), BF),
            pltpu.VMEM((half, dim_head, nfeat), BF),
            pltpu.VMEM((amount, width), BF),
            pltpu.SemaphoreType.DMA((4,)),
            pairs,
            turned,
            feat,
        ],
        2 * proj + feats,
        FIRST_LIMIT,
    )(place, flat, w_key, w_value, omega)
    (keep,) = call(
        second_kernel,
        [jax.ShapeDtypeStruct((2, rows, nfeat), F32)],
        [smem] + [vmem] * (2 + here),
        [pairs, turned, feat],
        feats,
    )(place, key, omega, *values)
    top = lax.ppermute(values[-1], "row", [(i, i + 1) for i in range(count - 1)])
    low = lax.ppermute(values[0], "row", [(i + 1, i) for i in range(count - 1)])
    (feat_query,) = call(
        query_kernel,
        [jax.ShapeDtypeStruct((amount, heads * nfeat), BF)],
        [vmem] * 3,
        [pltpu.VMEM((half, 2 * dim_head, 2 * nfeat), BF)],
        proj + feats,
    )(flat, w_query, omega)
    (base,) = call(
        conv_kernel_body,
        [jax.ShapeDtypeStruct((amount, width), F32)],
        [vmem] * (here + 5),
        [pltpu.VMEM((amount, width), BF)],
        proj,
    )(top, *values, low, flat, w_out, conv_kernel)
    mine = reduce_half(send, keep, count, split)
    theirs = swap(mine, 1, count)
    gain = norm_gain.reshape(1, width)
    part, square = call(
        own_kernel,
        [jax.ShapeDtypeStruct((amount, width), F32), jax.ShapeDtypeStruct((amount, 2 * dim_head), F32)],
        [smem] + [vmem] * 4,
        [mats],
        feats,
    )(place, mine, feat_query, gain, w_out)
    tile = tiles_of(amount, 256)
    (out,) = call(
        out_kernel,
        [jax.ShapeDtypeStruct((amount, width), BF)],
        [smem] + [vmem] * 7,
        [mats, pltpu.VMEM((amount, width), BF), pltpu.SemaphoreType.DMA((amount // tile,))],
        proj + feats,
        space=pltpu.HBM,
    )(place, theirs, feat_query, part, square, base, gain, w_out)
    return out.reshape(here, cols, width)


def solution(mesh):
    return jax.shard_map(
        layer,
        mesh=mesh,
        in_specs=(P(("parts", "row"), None, None), P(), P(), P(), P(), P(), P(), P()),
        out_specs=P(("parts", "row"), None, None),
        check_vma=False,
    )
```

```python
import math

import jax
import jax.numpy as jnp
from jax import lax
from jax.experimental import pallas as pl
from jax.experimental.pallas import tpu as pltpu
from jax.sharding import PartitionSpec as P


BF = jnp.bfloat16
F32 = jnp.float32
LOG2E = 1.4426950408889634
TILE = 256
VMEM_LIMIT = 28 * 1024 * 1024
FIRST_LIMIT = 54900000


def split_of(count):
    return min(4, count // 2)


def place_here():
    spot = lax.axis_index("row")
    shift = split_of(lax.axis_size("row")).bit_length() - 1
    return lax.bitwise_and(spot, 1), lax.bitwise_and(lax.shift_right_logical(spot, shift), 1)


def tiles_of(total, wanted):
    return wanted if total % wanted == 0 else total


def feature_tile(proj, omega_pair, dim_head, nfeat):
    lifted = jnp.dot(proj, omega_pair, preferred_element_type=F32)
    values = proj.astype(F32)
    square = values * values * (0.5 * dim_head ** (-0.5) * LOG2E)
    first = lax.broadcasted_iota(jnp.int32, square.shape, 1) < dim_head
    halves = []
    for head, mine in enumerate((jnp.where(first, square, 0.0), jnp.where(first, 0.0, square))):
        drop = jnp.sum(mine, axis=1, keepdims=True) + 0.5 * math.log2(nfeat)
        grown = lifted[:, head * nfeat : (head + 1) * nfeat] * (dim_head ** (-0.25) * LOG2E)
        halves.append(jnp.exp2(grown - drop).astype(BF))
    return jnp.concatenate(halves, axis=1)


def fill_pair(pair_ref, which, omegas):
    dim_head, nfeat = omegas[0].shape
    empty = jnp.zeros((dim_head, nfeat), BF)
    for side in range(2):
        rows = slice(side * dim_head, (side + 1) * dim_head)
        pair_ref[which, rows, side * nfeat : (side + 1) * nfeat] = omegas[side]
        pair_ref[which, rows, (1 - side) * nfeat : (2 - side) * nfeat] = empty


def fill_marks(vt_ref, group):
    heads, rows, tokens = vt_ref.shape
    mark = lax.broadcasted_iota(jnp.int32, (16, tokens), 0)
    for head in range(heads):
        vt_ref[head, rows - 16 :, :] = jnp.where(mark == head % group, 1.0, 0.0).astype(BF)


def half_state(bit, key_ref, offset, pair_ref, vt_ref, feat_ref, state_ref):
    heads, rows, tokens = vt_ref.shape
    dim_head = rows - 16
    wide = 2 * dim_head
    nfeat = feat_ref.shape[2] // 2
    group = heads // 2
    tile = tiles_of(tokens, TILE)
    sums = None
    for pair in range(heads // 2):
            lanes = slice(pair * wide, (pair + 1) * wide) if isinstance(offset, int) else pl.ds(pl.multiple_of(offset + pair * wide, wide), wide)
            for start in range(0, tokens, tile):
                feat_ref[pair, start : start + tile, :] = feature_tile(key_ref[start : start + tile, lanes], pair_ref[pair], dim_head, nfeat)
    for head in range(heads):
        pair, side = head // 2, head % 2
        local = jnp.dot(vt_ref[head], feat_ref[pair, :, side * nfeat : (side + 1) * nfeat], preferred_element_type=F32)
        slot = lax.rem(bit + head // group, 2)
        spot = head % group
        state_ref[slot, spot * dim_head : (spot + 1) * dim_head, :] = local[:dim_head].astype(state_ref.dtype)
        sums = local[dim_head:] if spot == 0 else sums + local[dim_head:]
        if spot == group - 1:
            state_ref[slot, group * dim_head :, :] = sums[:8].astype(state_ref.dtype)


def turn_values(value_refs, offset, span, vt_ref):
    heads, rows, _ = vt_ref.shape
    dim_head = rows - 16
    lanes = pl.ds(pl.multiple_of(offset, span), span)
    turned = jnp.concatenate([ref[:, lanes] for ref in value_refs], axis=0).T
    for head in range(heads):
        vt_ref[head, :dim_head, :] = turned[head * dim_head : (head + 1) * dim_head]


def first_kernel(x_hbm, wk_hbm, wv_hbm, omega_hbm, *refs):
    place = place_here()
    heads, _, _ = omega_hbm.shape
    tokens, width = x_hbm.shape
    here = len(refs) - 11
    send_ref, own_ref = refs[:2]
    value_refs = refs[2 : 2 + here]
    x_ref, wk_ref, wv_ref, omega_ref, key_ref, sems, pair_ref, vt_ref, feat_ref = refs[2 + here :]
    half, span = heads // 2, width // 2
    other = 1 - place[0]
    moves = [(x_hbm, x_ref), (wv_hbm, wv_ref), (omega_hbm.at[pl.ds(other * half, half)], omega_ref), (wk_hbm, wk_ref)]
    copies = [pltpu.make_async_copy(source, target, sems.at[i]) for i, (source, target) in enumerate(moves)]
    for copy in copies:
        copy.start()
    fill_marks(vt_ref, half // 2)
    cols = tokens // here
    blocks = [slice(row * cols, (row + 1) * cols) for row in range(here)]
    copies[0].wait()
    copies[1].wait()
    for block, value_ref in zip(blocks, value_refs):
        value_ref[...] = jnp.dot(x_ref[block, :], wv_ref[...], preferred_element_type=F32).astype(BF)
    copies[2].wait()
    for pair in range(half // 2):
        fill_pair(pair_ref, pair, [omega_ref[2 * pair], omega_ref[2 * pair + 1]])
    copies[3].wait()
    for block in blocks:
        key_ref[block, :] = jnp.dot(x_ref[block, :], wk_ref[...], preferred_element_type=F32).astype(BF)
    own_ref[...] = key_ref[:, pl.ds(pl.multiple_of(place[0] * span, span), span)]
    turn_values(value_refs, other * span, span, vt_ref)
    half_state(place[1], key_ref, other * span, pair_ref, vt_ref, feat_ref, send_ref)


def second_kernel(key_ref, omega_ref, *refs):
    place = place_here()
    heads, _, _ = omega_ref.shape
    value_refs = refs[:-4]
    state_ref, pair_ref, vt_ref, feat_ref = refs[-4:]
    half, span = heads // 2, key_ref.shape[1]
    core = place[0]
    fill_marks(vt_ref, half // 2)
    for pair in range(half // 2):
        fill_pair(pair_ref, pair, [omega_ref[core * half + 2 * pair], omega_ref[core * half + 2 * pair + 1]])
    turn_values(value_refs, core * span, span, vt_ref)
    half_state(place[1], key_ref, 0, pair_ref, vt_ref, feat_ref, state_ref)


def query_kernel(x_ref, wq_ref, omega_ref, feat_ref, pair_ref):
    heads, dim_head, nfeat = omega_ref.shape
    tokens = x_ref.shape[0]
    for pair in range(heads // 2):
        fill_pair(pair_ref, pair, [omega_ref[2 * pair], omega_ref[2 * pair + 1]])
    tile = tiles_of(tokens, TILE)
    for start in range(0, tokens, tile):
        query = jnp.dot(x_ref[start : start + tile, :], wq_ref[...], preferred_element_type=F32).astype(BF)
        for pair in range(heads // 2):
            proj = query[:, pair * 2 * dim_head : (pair + 1) * 2 * dim_head]
            feat_ref[start : start + tile, pair * 2 * nfeat : (pair + 1) * 2 * nfeat] = feature_tile(
                proj, pair_ref[pair], dim_head, nfeat
            )


def conv_kernel_body(*refs):
    x_ref, wo_ref, taps_ref, out_ref, pos_ref = refs[-5:]
    values = refs[:-5]
    here = len(values) - 2
    cols, width = values[0].shape
    lanes = 128
    col = lax.broadcasted_iota(jnp.int32, (cols, lanes), 0)
    for start in range(0, width, lanes):
        cut = slice(start, start + lanes)
        wide = [value[:, cut].astype(F32) for value in values]
        for row in range(here):
            sums = []
            for shift in range(3):
                terms = [wide[row + step] * taps_ref[step, shift : shift + 1, cut] for step in range(3)]
                sums.append(terms[0] + terms[1] + terms[2])
            left = jnp.where(col == 0, 0.0, pltpu.roll(sums[0], 1, 0))
            right = jnp.where(col == cols - 1, 0.0, pltpu.roll(sums[2], cols - 1, 0))
            pos_ref[row * cols : (row + 1) * cols, cut] = (left + sums[1] + right).astype(BF)
    for row in range(here):
        cut = slice(row * cols, (row + 1) * cols)
        out_ref[cut, :] = x_ref[cut, :].astype(F32) + jnp.dot(pos_ref[cut, :], wo_ref[...], preferred_element_type=F32)


def fill_mats(bit, state_ref, mat_ref, dim_head):
    pairs, _, both = mat_ref.shape
    nfeat = both // 2
    group = pairs
    wide = 2 * dim_head
    empty = jnp.zeros((dim_head, nfeat), BF)
    for head in range(2 * pairs):
        pair, side = head // 2, head % 2
        slot = lax.rem(bit + head // group, 2)
        spot = head % group
        mine, other = slice(side * nfeat, (side + 1) * nfeat), slice((1 - side) * nfeat, (2 - side) * nfeat)
        sums = state_ref[slot, group * dim_head :, :][spot : spot + 1]
        for base, block in (
            (0, state_ref[slot, spot * dim_head : (spot + 1) * dim_head, :]),
            (wide, jnp.broadcast_to(sums, (dim_head, nfeat))),
        ):
            rows = slice(base + side * dim_head, base + (side + 1) * dim_head)
            mat_ref[pair, rows, mine] = block
            mat_ref[pair, rows, other] = empty


def attend(feat, mat, wide):
    both = lax.dot_general(feat, mat, (((1,), (1,)), ((), ())), preferred_element_type=F32)
    return both[:, :wide] / both[:, wide:]


def own_kernel(state_ref, feat_ref, gain_ref, wo_ref, part_ref, square_ref, mat_ref):
    place = place_here()
    pairs, rows, _ = mat_ref.shape
    wide = rows // 2
    tokens = part_ref.shape[0]
    span = pairs * wide
    core = place[0]
    fill_mats(place[1], state_ref, mat_ref, wide // 2)
    tile = tiles_of(tokens, 256)
    for start in range(0, tokens, tile):
        cut = slice(start, start + tile)
        part_ref[cut, :], square_ref[cut, :] = half_share(core, span, feat_ref, cut, gain_ref, wo_ref, mat_ref)


def half_share(side, span, feat_ref, cut, gain_ref, wo_ref, mat_ref):
    pairs, rows, both = mat_ref.shape
    wide = rows // 2
    base = pl.multiple_of(side * span, span)
    total, scaled = None, []
    for pair in range(pairs):
        lanes = pl.ds(pl.multiple_of((side * pairs + pair) * both, both), both)
        attn = attend(feat_ref[cut, lanes], mat_ref[pair], wide)
        total = attn * attn if total is None else total + attn * attn
        gain = gain_ref[:, pl.ds(pl.multiple_of(base + pair * wide, wide), wide)]
        scaled.append((attn * gain).astype(BF))
    share = jnp.dot(jnp.concatenate(scaled, axis=1), wo_ref[pl.ds(base, span), :], preferred_element_type=F32)
    return share, total


def out_kernel(state_ref, feat_ref, part_ref, square_ref, base_ref, gain_ref, wo_ref, out_hbm, mat_ref, out_ref, sems):
    place = place_here()
    _, rows, _ = mat_ref.shape
    wide = rows // 2
    tokens, width = base_ref.shape
    fill_mats(place[1], state_ref, mat_ref, wide // 2)
    tile = tiles_of(tokens, 256)
    copies = []
    for start in range(0, tokens, tile):
        cut = slice(start, start + tile)
        share, total = half_share(1 - place[0], width // 2, feat_ref, cut, gain_ref, wo_ref, mat_ref)
        total = total + square_ref[cut, :]
        scale = lax.rsqrt(jnp.sum(total, axis=1, keepdims=True) * (1.0 / width) + 1e-06)
        out_ref[cut, :] = (base_ref[cut, :] + scale * (share + part_ref[cut, :])).astype(BF)
        copies.append(pltpu.make_async_copy(out_ref.at[cut], out_hbm.at[cut], sems.at[start // tile]))
        copies[-1].start()
    for copy in copies:
        copy.wait()


def call(kernel, out_shape, in_specs, scratch, flops, limit=VMEM_LIMIT, space=pltpu.VMEM):
    return pl.pallas_call(
        kernel,
        out_shape=out_shape,
        in_specs=in_specs,
        out_specs=[pl.BlockSpec(memory_space=space)] * len(out_shape),
        scratch_shapes=scratch,
        compiler_params=pltpu.CompilerParams(vmem_limit_bytes=limit),
        cost_estimate=pl.CostEstimate(flops=flops, bytes_accessed=0, transcendentals=0),
    )


def swap(block, bit, count):
    return lax.ppermute(block, "row", [(i, i ^ bit) for i in range(count)])


def reduce_half(send, keep, count, split):
    other = swap(send, 1, count)
    chip = keep + other.astype(F32)
    other = swap(chip[1].astype(BF), split, count)
    part = chip[0] + other.astype(F32)
    bit = count // 2
    while bit > 1:
        if bit != split:
            other = swap(part.astype(BF), bit, count)
            part = part + other.astype(F32)
        bit //= 2
    done = part.astype(BF)
    other = swap(done, split, count)
    return jnp.stack([done, other])


def layer(tokens, w_query, w_key, w_value, w_out, omega, conv_kernel, norm_gain):
    here, cols, width = tokens.shape
    heads, dim_head, nfeat = omega.shape
    count = lax.axis_size("row")
    split = split_of(count)
    flat = tokens.reshape(here * cols, width)
    amount = here * cols
    half, span = heads // 2, width // 2
    rows = half // 2 * dim_head + 8
    proj = 2 * amount * width * width
    feats = 2 * amount * width * nfeat
    vmem = pl.BlockSpec(memory_space=pltpu.VMEM)
    hbm = pl.BlockSpec(memory_space=pltpu.HBM)
    pairs = pltpu.VMEM((half // 2, 2 * dim_head, 2 * nfeat), BF)
    turned = pltpu.VMEM((half, dim_head + 16, amount), BF)
    feat = pltpu.VMEM((half // 2, amount, 2 * nfeat), BF)
    mats = pltpu.VMEM((half // 2, 4 * dim_head, 2 * nfeat), BF)

    send, key, *values = call(
        first_kernel,
        [jax.ShapeDtypeStruct((2, rows, nfeat), BF), jax.ShapeDtypeStruct((amount, span), BF)]
        + [jax.ShapeDtypeStruct((cols, width), BF)] * here,
        [hbm] * 4,
        [
            pltpu.VMEM((amount, width), BF),
            pltpu.VMEM((width, width), BF),
            pltpu.VMEM((width, width), BF),
            pltpu.VMEM((half, dim_head, nfeat), BF),
            pltpu.VMEM((amount, width), BF),
            pltpu.SemaphoreType.DMA((4,)),
            pairs,
            turned,
            feat,
        ],
        2 * proj + feats,
        FIRST_LIMIT,
    )(flat, w_key, w_value, omega)
    (keep,) = call(
        second_kernel,
        [jax.ShapeDtypeStruct((2, rows, nfeat), F32)],
        [vmem] * (2 + here),
        [pairs, turned, feat],
        feats,
    )(key, omega, *values)
    top = lax.ppermute(values[-1], "row", [(i, i + 1) for i in range(count - 1)])
    low = lax.ppermute(values[0], "row", [(i + 1, i) for i in range(count - 1)])
    (feat_query,) = call(
        query_kernel,
        [jax.ShapeDtypeStruct((amount, heads * nfeat), BF)],
        [vmem] * 3,
        [pltpu.VMEM((half, 2 * dim_head, 2 * nfeat), BF)],
        proj + feats,
    )(flat, w_query, omega)
    (base,) = call(
        conv_kernel_body,
        [jax.ShapeDtypeStruct((amount, width), F32)],
        [vmem] * (here + 5),
        [pltpu.VMEM((amount, width), BF)],
        proj,
    )(top, *values, low, flat, w_out, conv_kernel)
    mine = reduce_half(send, keep, count, split)
    theirs = swap(mine, 1, count)
    gain = norm_gain.reshape(1, width)
    part, square = call(
        own_kernel,
        [jax.ShapeDtypeStruct((amount, width), F32), jax.ShapeDtypeStruct((amount, 2 * dim_head), F32)],
        [vmem] * 4,
        [mats],
        feats,
    )(mine, feat_query, gain, w_out)
    tile = tiles_of(amount, 256)
    (out,) = call(
        out_kernel,
        [jax.ShapeDtypeStruct((amount, width), BF)],
        [vmem] * 7,
        [mats, pltpu.VMEM((amount, width), BF), pltpu.SemaphoreType.DMA((amount // tile,))],
        proj + feats,
        space=pltpu.HBM,
    )(theirs, feat_query, part, square, base, gain, w_out)
    return out.reshape(here, cols, width)


def solution(mesh):
    return jax.shard_map(
        layer,
        mesh=mesh,
        in_specs=(P(("parts", "row"), None, None), P(), P(), P(), P(), P(), P(), P()),
        out_specs=P(("parts", "row"), None, None),
        check_vma=False,
    )
```
